32 devices in a mesh: groups: 2 (over y), seq: 4 (over z), blk: 2 (over x), cfg: 2 (over core).
Axes of the slice: x: 2, y: 2, z: 4, core: 2. Of those that a mesh axis runs over, the one named last changes fastest.
Arguments:
- queries: bfloat16 [4, 320, 4096], P(('groups', 'cfg'), ('seq', 'blk')), parts along dimension 0, may hold values from -6 to 6
- keys: bfloat16 [4, 320, 4096], P(('groups', 'cfg'), ('seq', 'blk')), parts along dimension 0, may hold values from -6 to 6
- values: bfloat16 [4, 320, 4096], P(('groups', 'cfg'), ('seq', 'blk')), parts along dimension 0, may hold values from -6 to 6
- ref_keys: bfloat16 [4, 1024, 4096], P(('groups', 'cfg'), 'seq'), parts along dimension 0, may hold values from -6 to 6
- ref_values: bfloat16 [4, 1024, 4096], P(('groups', 'cfg'), 'seq'), parts along dimension 0, may hold values from -6 to 6
- ref_len: int32 [4], P(('groups', 'cfg')), parts along dimension 0, may hold values from 256 to 1024, as said below
- step_index: int32 [2], P('groups'), parts along dimension 0, may hold values from 0 to 49
- guide: float32 [2], P('groups'), parts along dimension 0, may hold values from 3 to 6
- latent: float32 [320, 128], P(('groups', 'seq', 'blk', 'cfg')), parts along dimension 0, may hold values from -6 to 6
- w_out: bfloat16 [4096, 64], replicated, may hold values from -1 to 1
Outputs:
- latent_next: float32 [320, 128], P(('groups', 'seq', 'blk', 'cfg')), parts along dimension 0
- denoised: float32 [320, 128], P(('groups', 'seq', 'blk', 'cfg')), parts along dimension 0
The draws below stay inside these ranges and needn't reach their ends.
There are 2 independent parts, one for each index of `groups`. The reference program is written for one: setup_inputs(seed, part) draws one part's arguments, and reference() takes and returns one part's arrays. A program takes and returns all parts, laid end to end along the dimension named above; an argument that names none is the same for every part. Nothing has to cross between parts.
Inputs may be any that keep to these rules, and one draw needn't show every extreme that they name: `ref_len`: one of the two branches has exactly 1024 valid reference tokens.
All inputs are finite; a program needn't handle non-finite values.
Results may differ from the reference program's by a relative error of at most 0.005.
Values may be sent and summed in bfloat16 or wider, within the bound.
No kernel may reach another device: no remote copies, remote signals or barrier semaphores. Data moves between devices by JAX's collectives and lax.ppermute only.
A program may use at most 128 MiB of HBM per device.

```python
import jax
import jax.numpy as jnp
from jax import lax

HEADS = 32
HD = 128
C_OUT = 64
STEPS = 50
REF = 1024
TOKENS = 320


def drawn_base(key, rows):
    width = HEADS * HD
    return jnp.clip(jax.random.normal(jax.random.fold_in(key, 1), (2, rows, width), jnp.float32), -5.0, 5.0)


def draw_queries(key, part):
    own = jax.random.fold_in(key, 101)
    result = drawn_base(own, TOKENS)
    return result.astype(jnp.bfloat16)


def draw_keys(key, part):
    own = jax.random.fold_in(key, 202)
    result = drawn_base(own, TOKENS)
    return result.astype(jnp.bfloat16)


def draw_ref_keys(key, part):
    own = jax.random.fold_in(key, 303)
    result = drawn_base(own, REF)
    return result.astype(jnp.bfloat16)


def draw_ref_len(key, part):
    which = jax.random.randint(jax.random.fold_in(key, 401), (), 0, 2)
    other = jax.random.randint(jax.random.fold_in(key, 402), (), REF // 4, REF + 1)
    return jnp.where(jnp.arange(2) == which, REF, other).astype(jnp.int32)


def steps_of(rng, extent, cuts, low, top_value):
    factor_of = 1.0
    for position, shards_of in cuts:
        steps = jax.random.uniform(jax.random.fold_in(jax.random.fold_in(rng, 6), position), (shards_of,), jnp.float32, low / len(cuts), top_value / len(cuts))
        factor_of = factor_of * jnp.repeat(jnp.exp(steps), extent[position] // shards_of).reshape((-1,) + (1,) * (len(extent) - 1 - position))
    return factor_of


def normal_values(key, shape, scale, bound, cuts=(), kind=jnp.bfloat16):
    loudness = steps_of(key, shape, cuts, -0.22, 0.18) if cuts else 1.0
    values = jax.random.normal(key, shape, jnp.float32) * scale * loudness
    return jnp.minimum(jnp.maximum(values, -bound), bound).astype(kind)


def setup_inputs(seed: int = 0, part: int = 0) -> dict:
    arg_keys = jax.random.split(jax.random.key(seed), 11)
    part_splits = jax.random.split(jax.random.fold_in(arg_keys[10], part), 11)
    queries = draw_queries(jax.random.fold_in(jax.random.fold_in(arg_keys[10], part), 71), part)
    keys = draw_keys(jax.random.fold_in(jax.random.fold_in(arg_keys[10], part), 71), part)
    values = normal_values(part_splits[2], (2, TOKENS, HEADS * HD), 1.0, 6.0, ((0, 2), (1, 8)))
    ref_keys = draw_ref_keys(jax.random.fold_in(jax.random.fold_in(arg_keys[10], part), 71), part)
    ref_values = normal_values(part_splits[4], (2, REF, HEADS * HD), 1.0, 6.0, ((0, 2), (1, 4)))
    ref_len = draw_ref_len(jax.random.fold_in(jax.random.fold_in(arg_keys[10], part), 71), part)
    step_index = jax.random.randint(part_splits[6], (1,), 0, STEPS).astype(jnp.int32)
    guide = jnp.clip(jax.random.uniform(part_splits[7], (1,), jnp.float32, 3.0, 6.0), 3.0, 6.0)
    latent = normal_values(part_splits[8], (TOKENS // 2, 2 * C_OUT), 1.0, 6.0, ((0, 16),), jnp.float32)
    w_out = normal_values(arg_keys[9], (HEADS * HD, C_OUT), (0.3 * (HEADS * HD) ** -0.5 * (TOKENS * REF * (TOKENS + REF) ** -1) ** 0.5), 1.0)
    return dict(queries=queries, keys=keys, values=values, ref_keys=ref_keys, ref_values=ref_values, ref_len=ref_len, step_index=step_index, guide=guide, latent=latent, w_out=w_out)


def head_attention(packed, length):
    query_head, key_head, value_head, refkey_head, refvalue_head = packed
    scale_factor = HD ** -0.5
    scores = jnp.dot(query_head, key_head.T, preferred_element_type=jnp.float32) * scale_factor
    top_score = jnp.max(scores, axis=1, keepdims=True)
    weights = jnp.exp(scores - top_score)
    self_out = jnp.dot(weights.astype(jnp.bfloat16), value_head, preferred_element_type=jnp.float32) / jnp.sum(weights, axis=1, keepdims=True)
    ref_scores = jnp.dot(query_head, refkey_head.T, preferred_element_type=jnp.float32) * scale_factor
    ref_index = jnp.arange(ref_scores.shape[1], dtype=jnp.int32)[None, :]
    ref_scores = jnp.where(ref_index < length, ref_scores, jnp.float32(-1e30))
    ref_top = jnp.max(ref_scores, axis=1, keepdims=True)
    ref_weights = jnp.exp(ref_scores - ref_top)
    ref_out = jnp.dot(ref_weights.astype(jnp.bfloat16), refvalue_head, preferred_element_type=jnp.float32) / jnp.sum(ref_weights, axis=1, keepdims=True)
    return self_out + ref_out


def branch_velocity(query_rows, key_rows, value_rows, refkey_rows, refvalue_rows, length, w_out):
    def split_heads(array):
        return array.reshape(array.shape[0], HEADS, HD).transpose(1, 0, 2)

    packed = (split_heads(query_rows), split_heads(key_rows), split_heads(value_rows), split_heads(refkey_rows), split_heads(refvalue_rows))
    outputs = lax.map(lambda item: head_attention(item, length), packed)
    attended = outputs.transpose(1, 0, 2).reshape(TOKENS, HEADS * HD).astype(jnp.bfloat16)
    velocity = jnp.dot(attended, w_out, preferred_element_type=jnp.float32)
    return velocity.reshape(TOKENS // 2, 2 * C_OUT)


def sigma_of(index):
    frac = 1.0 - index.astype(jnp.float32) / STEPS
    return 5.0 * frac / (1.0 + 4.0 * frac)


def reference(queries, keys, values, ref_keys, ref_values, ref_len, step_index, guide, latent, w_out):
    cond_vel = branch_velocity(queries[0], keys[0], values[0], ref_keys[0], ref_values[0], ref_len[0], w_out)
    uncond_vel = branch_velocity(queries[1], keys[1], values[1], ref_keys[1], ref_values[1], ref_len[1], w_out)
    guided = uncond_vel + guide[0] * (cond_vel - uncond_vel)
    sig_now = sigma_of(step_index[0])
    sig_next = sigma_of(step_index[0] + 1)
    latent_next = latent + (sig_next - sig_now) * guided
    denoised = latent - sig_now * guided
    return latent_next, denoised
```

```python
from functools import partial

import jax
import jax.numpy as jnp
from jax import lax
from jax.experimental import pallas as pl
from jax.experimental.pallas import tpu as pltpu
from jax.sharding import PartitionSpec as P

HD = 128
STEPS = 50
LOG2E = 1.4426950408889634


def swap(value, axis, mask):
    pairs = [(source, source ^ mask) for source in range(lax.axis_size(axis))]
    return lax.ppermute(value, axis, pairs)


def dot_t(left, right):
    return lax.dot_general(
        left, right, (((1,), (1,)), ((), ())), preferred_element_type=jnp.float32
    )


def stack_rows(scratch, refs):
    start = 0
    for ref in refs:
        rows = ref.shape[0]
        scratch[start : start + rows, :] = ref[...]
        start += rows


def attend_kernel(n_q, n_k, heads_step, valid_ref, *refs):
    q_refs = refs[:n_q]
    k_refs = refs[n_q : n_q + n_k]
    v_refs = refs[n_q + n_k : n_q + 2 * n_k]
    refk_ref, refv_ref, self_out, ref_out, lse_out, q_all, k_all, v_all, lse_all = refs[
        n_q + 2 * n_k :
    ]
    step = pl.program_id(0)
    stack_rows(q_all, q_refs)
    stack_rows(k_all, k_refs)
    stack_rows(v_all, v_refs)
    rows = q_all.shape[0]
    count = refk_ref.shape[0]
    total_heads = heads_step * pl.num_programs(0)
    lane = lax.broadcasted_iota(jnp.int32, (rows, 128), 1)
    masked = lax.broadcasted_iota(jnp.int32, (rows, count), 1) >= valid_ref[0]
    scale = HD ** (-0.5) * LOG2E

    @pl.when(step == 0)
    def _():
        lse_all[...] = jnp.zeros_like(lse_all)

    lse = lse_all[...]
    for head in range(heads_step):
        columns = slice(head * HD, (head + 1) * HD)
        query = q_all[:, columns]
        for which in range(2):
            if which == 0:
                scores = dot_t(query, k_all[:, columns]) * scale
                value = v_all[:, columns]
                out = self_out
            else:
                scores = dot_t(query, refk_ref[:, columns]) * scale
                scores = jnp.where(masked, jnp.float32(-1e30), scores)
                value = refv_ref[:, columns]
                out = ref_out
            top = jnp.max(scores, axis=1, keepdims=True)
            weights = jnp.exp2(scores - top)
            total = jnp.sum(weights, axis=1, keepdims=True)
            summed = jnp.dot(
                weights.astype(jnp.bfloat16), value, preferred_element_type=jnp.float32
            )
            out[:, columns] = (summed / total).astype(out.dtype)
            column = step * heads_step + head + which * (128 // 4)
            lse = jnp.where(lane == column, top + jnp.log2(total), lse)
    lse_all[...] = lse

    @pl.when(step == pl.num_programs(0) - 1)
    def _():
        half = rows // 2
        low = lax.broadcasted_iota(jnp.int32, (half, 128), 1) < 64
        lse_out[...] = jnp.where(low, lse[:half], pltpu.roll(lse[half:], 64, 1))


def attend(q_parts, k_parts, v_parts, refkey, refvalue, valid):
    rows = sum(part.shape[0] for part in q_parts)
    keys = sum(part.shape[0] for part in k_parts)
    count, width = refkey.shape
    heads = width // HD
    heads_step = 4
    steps = heads // heads_step
    columns = heads_step * HD

    def block(array):
        return pl.BlockSpec((array.shape[0], columns), lambda i: (0, i))

    arrays = (*q_parts, *k_parts, *v_parts, refkey, refvalue)
    return pl.pallas_call(
        partial(attend_kernel, len(q_parts), len(k_parts), heads_step),
        grid=(steps,),
        in_specs=[pl.BlockSpec(memory_space=pltpu.SMEM)] + [block(a) for a in arrays],
        out_specs=[
            pl.BlockSpec((rows, columns), lambda i: (0, i)),
            pl.BlockSpec((rows, columns), lambda i: (0, i)),
            pl.BlockSpec((rows // 2, 128), lambda i: (0, 0)),
        ],
        out_shape=[
            jax.ShapeDtypeStruct((rows, width), jnp.float32),
            jax.ShapeDtypeStruct((rows, width), jnp.float32),
            jax.ShapeDtypeStruct((rows // 2, 128), jnp.float32),
        ],
        scratch_shapes=[
            pltpu.VMEM((rows, columns), jnp.bfloat16),
            pltpu.VMEM((keys, columns), jnp.bfloat16),
            pltpu.VMEM((keys, columns), jnp.bfloat16),
            pltpu.VMEM((rows, 128), jnp.float32),
        ],
        compiler_params=pltpu.CompilerParams(dimension_semantics=("arbitrary",)),
        cost_estimate=pl.CostEstimate(
            flops=4 * rows * (keys + count) * width,
            bytes_accessed=4 * (keys + count) * width + 10 * rows * width,
            transcendentals=rows * (keys + count) * heads,
        ),
        name="attend",
    )(valid, *arrays)


def project_kernel(heads, n_other, factor_ref, own_ref, *refs):
    other_refs = refs[:n_other]
    self_ref, part_ref, w_ref, out_ref, merged, pairs = refs[n_other:]
    own = own_ref[...]
    half = own.shape[0]
    others = []
    if n_other == 3:
        quarter = half // 2
        for mask, ref in zip((1, 2, 3), other_refs):
            value = ref[...]
            if mask & 1:
                value = jnp.concatenate([value[quarter:], value[:quarter]], axis=0)
            if mask & 2:
                value = pltpu.roll(value, 64, 1)
            others.append(value)
        everyone = [own] + others
    else:
        everyone = [other_refs[0][i] for i in range(other_refs[0].shape[0])]
    top = everyone[0]
    for value in everyone[1:]:
        top = jnp.maximum(top, value)
    total = jnp.exp2(everyone[0] - top)
    for value in everyone[1:]:
        total = total + jnp.exp2(value - top)
    share = jnp.exp2(own - top) / total
    for head in range(heads):
        columns = slice(head * HD, (head + 1) * HD)
        for part in range(2):
            rows = slice(part * half, (part + 1) * half)
            base = part * 64 + head
            value = self_ref[rows, columns] * share[:, base : base + 1]
            value += part_ref[rows, columns] * share[:, base + 32 : base + 33]
            merged[rows, columns] = value.astype(jnp.bfloat16)
    weight = jnp.concatenate([w_ref[...], w_ref[...]], axis=0)
    velocity = dot_t(merged[...], weight)
    row = lax.broadcasted_iota(jnp.int32, velocity.shape, 0)
    lane = lax.broadcasted_iota(jnp.int32, velocity.shape, 1)
    keep = (row % 2 == 0) == (lane < 64)
    pairs[...] = jnp.where(keep, velocity * factor_ref[0], 0.0)
    out_ref[...] = pairs[pl.ds(0, half, stride=2), :] + pairs[pl.ds(1, half, stride=2), :]


def project(factor, own, others, self_part, ref_part, w_t):
    rows, width = self_part.shape
    vmem = pl.BlockSpec(memory_space=pltpu.VMEM)
    return pl.pallas_call(
        partial(project_kernel, width // HD, len(others)),
        in_specs=[pl.BlockSpec(memory_space=pltpu.SMEM)] + [vmem] * (4 + len(others)),
        out_specs=vmem,
        out_shape=jax.ShapeDtypeStruct((rows // 2, 128), jnp.float32),
        scratch_shapes=[
            pltpu.VMEM((rows, width), jnp.bfloat16),
            pltpu.VMEM((rows, 128), jnp.float32),
        ],
        cost_estimate=pl.CostEstimate(
            flops=4 * rows * width * 64, bytes_accessed=8 * rows * width, transcendentals=0
        ),
        name="project",
    )(factor, own, *others, self_part, ref_part, w_t)


def sigma_of(index):
    frac = 1.0 - index.astype(jnp.float32) / STEPS
    return 5.0 * frac / (1.0 + 4.0 * frac)


def gather_queries(own):
    if lax.axis_size("seq") != 4:
        return [lax.all_gather(own, "seq", axis=0, tiled=True)]
    far = swap(own, "seq", 3)
    near = swap(own, "seq", 1)
    place = lax.axis_index("seq")
    inner = jnp.logical_or(place == 1, place == 2)
    onward = jnp.where(inner, far, own)
    middle = lax.ppermute(onward, "seq", [(0, 2), (2, 3), (3, 1), (1, 0)])
    return [own, near, middle, far]


def gather_block(own):
    if lax.axis_size("blk") != 2:
        return [lax.all_gather(own, "blk", axis=0, tiled=True)]
    return [own, swap(own, "blk", 1)]


def on_device(
    queries, keys, values, ref_keys, ref_values, ref_len, step_index, guide, latent, w_out
):
    line = lax.axis_size("seq")
    place = lax.axis_index("seq")
    q_parts = gather_queries(queries[0])
    k_parts = gather_block(keys[0])
    v_parts = gather_block(values[0])
    valid = ref_len - place * ref_keys.shape[1]
    self_part, ref_part, lse = attend(
        q_parts, k_parts, v_parts, ref_keys[0], ref_values[0], valid
    )
    if line == 4:
        others = [swap(lse, "seq", mask) for mask in (1, 2, 3)]
    else:
        others = [lax.all_gather(lse, "seq", axis=0, tiled=False)]
    branch = lax.axis_index("cfg")
    factor = jnp.where(branch == 0, guide, 1.0 - guide)
    velocity = project(factor, lse, others, self_part, ref_part, w_out.T)
    blocks = velocity.reshape(line, -1, velocity.shape[1])
    if line == 4:
        parts = [blocks[0]] + [swap(blocks[mask], "seq", mask) for mask in (1, 2, 3)]
        mine = (parts[0] + parts[1]) + (parts[2] + parts[3])
    else:
        mine = lax.all_to_all(blocks, "seq", split_axis=0, concat_axis=0, tiled=True).sum(0)
    half_rows = mine.shape[0] // 2
    kept = lax.dynamic_slice_in_dim(mine, branch * half_rows, half_rows, 0)
    given = lax.dynamic_slice_in_dim(mine, (1 - branch) * half_rows, half_rows, 0)
    guided = kept + swap(given, "cfg", 1)
    sig_now = sigma_of(step_index[0])
    sig_next = sigma_of(step_index[0] + 1)
    latent_next = latent + (sig_next - sig_now) * guided
    denoised = latent - sig_now * guided
    return (latent_next, denoised)


def solution(mesh):
    in_specs = (
        P(("groups", "cfg"), ("seq", "blk"), None),
        P(("groups", "cfg"), ("seq", "blk"), None),
        P(("groups", "cfg"), ("seq", "blk"), None),
        P(("groups", "cfg"), "seq", None),
        P(("groups", "cfg"), "seq", None),
        P(("groups", "cfg")),
        P("groups"),
        P("groups"),
        P(("groups", "seq", "blk", "cfg"), None),
        P(),
    )
    out_specs = (P(("groups", "seq", "blk", "cfg"), None), P(("groups", "seq", "blk", "cfg"), None))
    return jax.shard_map(
        on_device, mesh=mesh, in_specs=in_specs, out_specs=out_specs, check_vma=False
    )
```

```python
from functools import partial

import jax
import jax.numpy as jnp
from jax import lax
from jax.experimental import pallas as pl
from jax.experimental.pallas import tpu as pltpu
from jax.sharding import PartitionSpec as P

HD = 128
STEPS = 50
LOG2E = 1.4426950408889634
NEG = -1e30

SMEM = pl.BlockSpec(memory_space=pltpu.SMEM)
VMEM = pl.BlockSpec(memory_space=pltpu.VMEM)


def in_vmem(array):
    return pltpu.with_memory_space_constraint(array, pltpu.VMEM)


def in_hbm(array):
    return pltpu.with_memory_space_constraint(array, pltpu.HBM)


def dot_t(left, right):
    return lax.dot_general(
        left, right, (((1,), (1,)), ((), ())), preferred_element_type=jnp.float32
    )


def exchange(value, axis, pairs):
    return lax.ppermute(value, axis, pairs)


def swap(value, axis, mask):
    return exchange(value, axis, [(i, i ^ mask) for i in range(lax.axis_size(axis))])


def head_columns(head):
    return slice(head * HD, (head + 1) * HD)


def partials(query, keys, values, refkeys, refvalues, weight, valid, out, heads, group):
    rows = query.shape[0]
    masked = lax.broadcasted_iota(jnp.int32, (rows, refkeys.shape[0]), 1) >= valid
    lane = lax.broadcasted_iota(jnp.int32, (rows, 128), 1)
    scale = HD ** (-0.5) * LOG2E
    lse = jnp.zeros((rows, 128), jnp.float32)
    for first in range(0, heads, group):
        some = range(first, first + group)
        scores, tops, weights, totals, outs = {}, {}, {}, {}, {}
        for h in some:
            columns = head_columns(h)
            scores[h, 0] = dot_t(query[:, columns], keys[:, columns])
            found = dot_t(query[:, columns], refkeys[:, columns])
            scores[h, 1] = jnp.where(masked, jnp.float32(NEG), found)
        for item, score in scores.items():
            tops[item] = jnp.max(score, axis=1, keepdims=True)
        for item, score in scores.items():
            weights[item] = jnp.exp2((score - tops[item]) * scale)
        for item in scores:
            totals[item] = jnp.sum(weights[item], axis=1, keepdims=True)
        for h in some:
            for which, value in ((0, values), (1, refvalues)):
                outs[h, which] = jnp.dot(
                    weights[h, which].astype(jnp.bfloat16),
                    value[:, head_columns(h)],
                    preferred_element_type=jnp.float32,
                )
        for h in some:
            both = [outs[h, w] * (1.0 / totals[h, w]) for w in range(2)]
            both = jnp.concatenate([part.astype(jnp.bfloat16) for part in both], axis=1)
            out[:, head_columns(h)] = dot_t(both, weight[:, 2 * h * HD : 2 * (h + 1) * HD])
        for h, which in scores:
            value = tops[h, which] * scale + jnp.log2(totals[h, which])
            lse = jnp.where(lane == which * 32 + h, value, lse)
    return lse


def fill_rows(scratch, refs):
    start = 0
    for ref in refs:
        scratch[start : start + ref.shape[0], :] = ref[...]
        start += ref.shape[0]


def fill_weight(weight, w_ref, heads):
    weight[...] = jnp.zeros_like(weight)
    out = w_ref.shape[0]
    for h in range(heads):
        weight[:out, 2 * h * HD : (2 * h + 1) * HD] = w_ref[:, head_columns(h)]
        weight[out:, (2 * h + 1) * HD : 2 * (h + 1) * HD] = w_ref[:, head_columns(h)]


def is_inner():
    place = lax.axis_index("seq")
    return jnp.logical_or(place == 1, place == 2)


def load_kernel(heads, ref_len, step_index, guide, *refs):
    sources, w_ref, valid, scalars, targets, weight, w_here, sems = (
        refs[:5], refs[5], refs[6], refs[7], refs[8:13], refs[13], refs[14], refs[15]
    )
    copies = [
        pltpu.make_async_copy(source, target, sems.at[i])
        for i, (source, target) in enumerate(zip((w_ref, *sources), (w_here, *targets)))
    ]
    for copy in copies:
        copy.start()
    valid[0] = ref_len[0] - lax.axis_index("seq") * sources[3].shape[0]
    scalars[0] = jnp.where(lax.axis_index("cfg") == 0, guide[0], 1.0 - guide[0])
    sig_now = sigma_of(step_index[0])
    scalars[1] = sig_now
    scalars[2] = sigma_of(step_index[0] + 1) - sig_now
    copies[0].wait()
    fill_weight(weight, w_here, heads)
    for copy in copies[1:]:
        copy.wait()


def onward_kernel(far_in, own, out):
    @pl.when(is_inner())
    def _():
        out[...] = far_in[...]

    @pl.when(jnp.logical_not(is_inner()))
    def _():
        out[...] = own[...]


def early_kernel(
    heads, group, valid, own, near, far_in, far_out, k0, k1, v0, v1, refk, refv, weight,
    out, lse, keys, values, query,
):
    count = own.shape[0]
    query[:count] = own[...]
    query[count : 2 * count] = near[...]

    @pl.when(is_inner())
    def _():
        query[2 * count :] = far_in[...]

    @pl.when(jnp.logical_not(is_inner()))
    def _():
        query[2 * count :] = far_out[...]

    fill_rows(keys, (k0, k1))
    fill_rows(values, (v0, v1))
    lse[...] = partials(query, keys, values, refk, refv, weight, valid[0], out, heads, group)


def late_kernel(
    heads, group, valid, query, keys, values, refk, refv, weight, lse_early, out, lse
):
    count = query.shape[0]
    middle = partials(query, keys, values, refk, refv, weight, valid[0], out, heads, group)
    low = lax.broadcasted_iota(jnp.int32, middle.shape, 1) < 64
    early = lse_early[...]
    lse[:count] = jnp.where(low, early[:count], pltpu.roll(middle, 64, 1))
    lse[count:] = jnp.where(
        low, early[count : 2 * count], pltpu.roll(early[2 * count :], 64, 1)
    )


def weigh(parts, shares, heads):
    rows = shares.shape[0]
    low = lax.broadcasted_iota(jnp.int32, (rows, 128), 1) < 64
    sums = [None] * 4
    for h in range(heads):
        index = jnp.where(low, h, 32 + h)
        value = parts[:, head_columns(h)] * jnp.take_along_axis(shares, index, axis=1)
        sums[h % 4] = value if sums[h % 4] is None else sums[h % 4] + value
    total = (sums[0] + sums[1]) + (sums[2] + sums[3])
    return total + pltpu.roll(total, 64, 1)


def pair_rows(velocity, factor, pairs):
    row = lax.broadcasted_iota(jnp.int32, velocity.shape, 0)
    low = lax.broadcasted_iota(jnp.int32, velocity.shape, 1) < 64
    pairs[...] = jnp.where((row % 2 == 0) == low, velocity * factor, 0.0)


def share_of(own, everyone):
    top = everyone[0]
    for value in everyone[1:]:
        top = jnp.maximum(top, value)
    total = jnp.exp2(everyone[0] - top)
    for value in everyone[1:]:
        total = total + jnp.exp2(value - top)
    return jnp.exp2(own - top) * (1.0 / total)


def combine_kernel(heads, factor, own, o1, o2, o3, early, late, b0, b1, b2, b3, pairs):
    count = late.shape[0]
    everyone = [own[...]]
    for mask, ref in ((1, o1), (2, o2), (3, o3)):
        value = ref[...]
        if mask & 1:
            value = jnp.concatenate([value[count:], value[:count]], axis=0)
        if mask & 2:
            value = pltpu.roll(value, 64, 1)
        everyone.append(value)
    share = share_of(everyone[0], everyone)
    turned = pltpu.roll(share, 64, 1)
    placed = (
        (early[:count], share[:count]),
        (early[count : 2 * count], share[count:]),
        (late[...], turned[:count]),
        (early[2 * count :], turned[count:]),
    )
    for (parts, shares), block in zip(placed, (b0, b1, b2, b3)):
        pair_rows(weigh(parts, shares, heads), factor[0], pairs)
        rows = block.shape[0]
        block[...] = pairs[pl.ds(0, rows, stride=2), :] + pairs[pl.ds(1, rows, stride=2), :]


def estimate(rows, keys, width):
    return pl.CostEstimate(
        flops=4 * rows * keys * width + 4 * rows * width * 128,
        bytes_accessed=4 * keys * width,
        transcendentals=rows * keys * width // HD,
    )


def vmem_params(mib):
    return pltpu.CompilerParams(vmem_limit_bytes=mib << 20)


def split_kernel(b0, r1, r2, r3, kept, given):
    total = (b0[...] + r1[...]) + (r2[...] + r3[...])
    half = total.shape[0] // 2
    first = lax.axis_index("cfg") == 0
    kept[...] = jnp.where(first, total[:half], total[half:])
    given[...] = jnp.where(first, total[half:], total[:half])


def euler_kernel(scalars, latent, kept, taken, latent_next, denoised):
    guided = kept[...] + taken[...]
    latent_next[...] = latent[...] + scalars[2] * guided
    denoised[...] = latent[...] - scalars[1] * guided


def line_of_four(
    query, keys, values, refk, refv, ref_len, step_index, guide, latent, w_t
):
    count, width = query.shape
    heads = width // HD
    rest = refk.shape[0] + 2 * count
    sources = (query, keys, values, refk, refv)
    valid, scalars, query_here, keys_here, values_here, refk, refv, weight = pl.pallas_call(
        partial(load_kernel, heads),
        in_specs=[SMEM] * 3 + [pl.BlockSpec(memory_space=pltpu.HBM)] * 6,
        out_specs=[SMEM] * 2 + [VMEM] * 6,
        out_shape=[jax.ShapeDtypeStruct((1,), jnp.int32), jax.ShapeDtypeStruct((3,), jnp.float32)]
        + [pltpu.VMEM(a.shape, a.dtype) for a in sources]
        + [pltpu.VMEM((128, 2 * width), jnp.bfloat16)],
        scratch_shapes=[pltpu.VMEM(w_t.shape, w_t.dtype), pltpu.SemaphoreType.DMA((6,))],
        compiler_params=vmem_params(2),
        cost_estimate=pl.CostEstimate(
            flops=10000000, bytes_accessed=4 * (refk.size + query.size), transcendentals=0
        ),
        name="load",
    )(ref_len, step_index, guide, *[in_hbm(a) for a in (*sources, w_t)])
    far_in = exchange(query, "seq", [(1, 2), (2, 1)])
    near = swap(query, "seq", 1)
    k_other = swap(keys, "blk", 1)
    v_other = swap(values, "blk", 1)
    far_out = exchange(query, "seq", [(0, 3), (3, 0)])
    onward = pl.pallas_call(
        onward_kernel,
        in_specs=[VMEM] * 2,
        out_specs=VMEM,
        out_shape=pltpu.VMEM(query.shape, query.dtype),
        compiler_params=vmem_params(2),
        name="onward",
    )(in_vmem(far_in), in_vmem(query_here))
    middle = exchange(onward, "seq", [(0, 2), (2, 3), (3, 1), (1, 0)])
    arrays = (
        query_here, near, far_in, far_out, keys_here, k_other, values_here, v_other,
        refk, refv, weight,
    )
    out_e, lse_e, k_all, v_all = pl.pallas_call(
        partial(early_kernel, heads, 8),
        in_specs=[SMEM] + [VMEM] * len(arrays),
        out_specs=[VMEM] * 4,
        out_shape=[
            pltpu.VMEM((3 * count, width), jnp.float32),
            pltpu.VMEM((3 * count, 128), jnp.float32),
            pltpu.VMEM((2 * count, width), jnp.bfloat16),
            pltpu.VMEM((2 * count, width), jnp.bfloat16),
        ],
        scratch_shapes=[pltpu.VMEM((3 * count, width), jnp.bfloat16)],
        compiler_params=vmem_params(12),
        cost_estimate=estimate(3 * count, rest, width),
        name="early",
    )(valid, *[in_vmem(a) for a in arrays])
    arrays = (middle, k_all, v_all, refk, refv, weight, lse_e)
    out_l, lse = pl.pallas_call(
        partial(late_kernel, heads, 16),
        in_specs=[SMEM] + [VMEM] * len(arrays),
        out_specs=[VMEM] * 2,
        out_shape=[
            pltpu.VMEM((count, width), jnp.float32),
            pltpu.VMEM((2 * count, 128), jnp.float32),
        ],
        compiler_params=vmem_params(12),
        cost_estimate=estimate(count, rest, width),
        name="late",
    )(valid, *[in_vmem(a) for a in arrays])
    arrays = [lse] + [swap(lse, "seq", mask) for mask in (1, 2, 3)] + [out_e, out_l]
    blocks = pl.pallas_call(
        partial(combine_kernel, heads),
        in_specs=[SMEM] + [VMEM] * len(arrays),
        out_specs=[VMEM] * 4,
        out_shape=[pltpu.VMEM((count // 2, 128), jnp.float32)] * 4,
        scratch_shapes=[pltpu.VMEM((count, 128), jnp.float32)],
        compiler_params=vmem_params(12),
        name="combine",
    )(scalars, *[in_vmem(a) for a in arrays])
    parts = [blocks[0]] + [swap(blocks[mask], "seq", mask) for mask in (1, 2, 3)]
    kept, given = pl.pallas_call(
        split_kernel,
        in_specs=[VMEM] * 4,
        out_specs=[VMEM] * 2,
        out_shape=[pltpu.VMEM(latent.shape, latent.dtype)] * 2,
        compiler_params=vmem_params(2),
        name="split",
    )(*[in_vmem(a) for a in parts])
    taken = swap(given, "cfg", 1)
    return pl.pallas_call(
        euler_kernel,
        in_specs=[SMEM] + [VMEM] * 3,
        out_specs=[VMEM] * 2,
        out_shape=[jax.ShapeDtypeStruct(latent.shape, latent.dtype)] * 2,
        compiler_params=vmem_params(2),
        name="euler",
    )(scalars, *[in_vmem(a) for a in (latent, kept, taken)])


def attend_kernel(heads, valid, query, keys, values, refk, refv, w_ref, out, lse, weight, total):
    step = pl.program_id(0)
    fill_weight(weight, w_ref, heads)

    @pl.when(step == 0)
    def _():
        total[...] = jnp.zeros_like(total)

    found = partials(query, keys, values, refk, refv, weight, valid[0], out, heads, 1)
    lane = lax.broadcasted_iota(jnp.int32, found.shape, 1)
    for h in range(heads):
        for column in (h, 32 + h):
            here = lane == step * heads + column
            total[...] = jnp.where(here, found[:, column : column + 1], total[...])

    @pl.when(step == pl.num_programs(0) - 1)
    def _():
        lse[...] = total[...]


def combine_any_kernel(heads, factor, own, everyone, parts, out, pairs):
    values = [everyone[i] for i in range(everyone.shape[0])]
    share = share_of(own[...], values)
    pair_rows(weigh(parts, share, heads), factor[0], pairs)
    rows = out.shape[0]
    out[...] = pairs[pl.ds(0, rows, stride=2), :] + pairs[pl.ds(1, rows, stride=2), :]


def any_line(
    query, keys, values, refk, refv, ref_len, step_index, guide, latent, w_t
):
    line = lax.axis_size("seq")
    valid = ref_len - lax.axis_index("seq") * refk.shape[0]
    branch = lax.axis_index("cfg")
    factor = jnp.where(branch == 0, guide, 1.0 - guide)
    query = lax.all_gather(query, "seq", axis=0, tiled=True)
    keys = lax.all_gather(keys, "blk", axis=0, tiled=True)
    values = lax.all_gather(values, "blk", axis=0, tiled=True)
    rows, width = query.shape
    heads = width // HD
    some = 4
    columns = some * HD
    arrays = (query, keys, values, refk, refv, w_t)
    out, lse = pl.pallas_call(
        partial(attend_kernel, some),
        grid=(heads // some,),
        in_specs=[SMEM]
        + [pl.BlockSpec((a.shape[0], columns), lambda i: (0, i)) for a in arrays],
        out_specs=[
            pl.BlockSpec((rows, columns), lambda i: (0, i)),
            pl.BlockSpec((rows, 128), lambda i: (0, 0)),
        ],
        out_shape=[
            jax.ShapeDtypeStruct((rows, width), jnp.float32),
            jax.ShapeDtypeStruct((rows, 128), jnp.float32),
        ],
        scratch_shapes=[
            pltpu.VMEM((128, 2 * columns), jnp.bfloat16),
            pltpu.VMEM((rows, 128), jnp.float32),
        ],
        compiler_params=pltpu.CompilerParams(dimension_semantics=("arbitrary",)),
        name="attend",
    )(valid, *arrays)
    everyone = lax.all_gather(lse, "seq", axis=0, tiled=False)
    velocity = pl.pallas_call(
        partial(combine_any_kernel, heads),
        in_specs=[SMEM] + [VMEM] * 3,
        out_specs=VMEM,
        out_shape=jax.ShapeDtypeStruct((rows // 2, 128), jnp.float32),
        scratch_shapes=[pltpu.VMEM((rows, 128), jnp.float32)],
        name="combine",
    )(factor, lse, everyone, out)
    blocks = velocity.reshape(line, -1, 128)
    mine = lax.all_to_all(blocks, "seq", split_axis=0, concat_axis=0, tiled=True).sum(0)
    half_rows = mine.shape[0] // 2
    kept = lax.dynamic_slice_in_dim(mine, branch * half_rows, half_rows, 0)
    given = lax.dynamic_slice_in_dim(mine, (1 - branch) * half_rows, half_rows, 0)
    guided = kept + swap(given, "cfg", 1)
    sig_now = sigma_of(step_index[0])
    sig_next = sigma_of(step_index[0] + 1)
    return (latent + (sig_next - sig_now) * guided, latent - sig_now * guided)


def sigma_of(index):
    frac = 1.0 - index.astype(jnp.float32) / STEPS
    return 5.0 * frac / (1.0 + 4.0 * frac)


def on_device(
    queries, keys, values, ref_keys, ref_values, ref_len, step_index, guide, latent, w_out
):
    special = lax.axis_size("seq") == 4 and lax.axis_size("blk") == 2
    return tuple(
        (line_of_four if special else any_line)(
            queries[0], keys[0], values[0], ref_keys[0], ref_values[0],
            ref_len, step_index, guide, latent, w_out.T,
        )
    )


def solution(mesh):
    in_specs = (
        P(("groups", "cfg"), ("seq", "blk"), None),
        P(("groups", "cfg"), ("seq", "blk"), None),
        P(("groups", "cfg"), ("seq", "blk"), None),
        P(("groups", "cfg"), "seq", None),
        P(("groups", "cfg"), "seq", None),
        P(("groups", "cfg")),
        P("groups"),
        P("groups"),
        P(("groups", "seq", "blk", "cfg"), None),
        P(),
    )
    out_specs = (P(("groups", "seq", "blk", "cfg"), None), P(("groups", "seq", "blk", "cfg"), None))
    return jax.shard_map(
        on_device, mesh=mesh, in_specs=in_specs, out_specs=out_specs, check_vma=False
    )
```

```python
from functools import partial

import jax
import jax.numpy as jnp
from jax import lax
from jax.experimental import pallas as pl
from jax.experimental.pallas import tpu as pltpu
from jax.sharding import PartitionSpec as P

HD = 128
STEPS = 50
LOG2E = 1.4426950408889634
NEG = -1e30
SCALE = HD ** (-0.5) * LOG2E

SMEM = pl.BlockSpec(memory_space=pltpu.SMEM)
VMEM = pl.BlockSpec(memory_space=pltpu.VMEM)


def in_vmem(array):
    return pltpu.with_memory_space_constraint(array, pltpu.VMEM)


def in_hbm(array):
    return pltpu.with_memory_space_constraint(array, pltpu.HBM)


def dot_t(left, right):
    return lax.dot_general(
        left, right, (((1,), (1,)), ((), ())), preferred_element_type=jnp.float32
    )


def exchange(value, axis, pairs):
    return lax.ppermute(value, axis, pairs)


def swap(value, axis, mask):
    return exchange(value, axis, [(i, i ^ mask) for i in range(lax.axis_size(axis))])


def head_columns(head):
    return slice(head * HD, (head + 1) * HD)


def head_scores(query, keys, refkeys, bias, some):
    scores = {}
    for h in some:
        columns = head_columns(h)
        scores[h, 0] = dot_t(query[:, columns], keys[:, columns])
        scores[h, 1] = dot_t(query[:, columns], refkeys[:, columns]) + bias
    return scores


def head_exps(scores):
    tops = {item: jnp.max(score, axis=1, keepdims=True) for item, score in scores.items()}
    exps = {item: jnp.exp2((score - tops[item]) * SCALE) for item, score in scores.items()}
    totals = {item: jnp.sum(exps[item], axis=1, keepdims=True) for item in scores}
    return tops, exps, totals


def place_columns(target, lane, columns):
    for (h, which), column in columns.items():
        target = jnp.where(lane == which * 32 + h, column, target)
    return target


def head_outputs(exps, values, refvalues, some):
    return {
        h: jnp.concatenate(
            [
                jnp.dot(
                    exps[h, which], value[:, head_columns(h)], preferred_element_type=jnp.float32
                ).astype(jnp.bfloat16)
                for which, value in ((0, values), (1, refvalues))
            ],
            axis=1,
        )
        for h in some
    }


def fill_rows(scratch, refs):
    start = 0
    for ref in refs:
        scratch[start : start + ref.shape[0], :] = ref[...]
        start += ref.shape[0]


def fill_weight(weight, w_ref, heads):
    weight[...] = jnp.zeros_like(weight)
    out = w_ref.shape[0]
    for h in range(heads):
        weight[:out, 2 * h * HD : (2 * h + 1) * HD] = w_ref[:, head_columns(h)]
        weight[out:, (2 * h + 1) * HD : 2 * (h + 1) * HD] = w_ref[:, head_columns(h)]


def is_inner():
    place = lax.axis_index("seq")
    return jnp.logical_or(place == 1, place == 2)


def is_inner():
    place = lax.axis_index("seq")
    return jnp.logical_or(place == 1, place == 2)


def sigma_of(index):
    frac = 1.0 - index.astype(jnp.float32) / STEPS
    return 5.0 * frac / (1.0 + 4.0 * frac)


def load_kernel(heads, ref_len, step_index, guide, *refs):
    sources, w_ref, bias, scalars, targets, weight, w_here, sems = (
        refs[:5], refs[5], refs[6], refs[7], refs[8:13], refs[13], refs[14], refs[15]
    )
    copies = [
        pltpu.make_async_copy(source, target, sems.at[i])
        for i, (source, target) in enumerate(zip((w_ref, *sources), (w_here, *targets)))
    ]
    for copy in copies:
        copy.start()
    valid = ref_len[0] - lax.axis_index("seq") * sources[3].shape[0]
    index = lax.broadcasted_iota(jnp.int32, bias.shape, 1)
    bias[...] = jnp.where(index < valid, 0.0, jnp.float32(NEG))
    sig_now = sigma_of(step_index[0])
    factor = jnp.where(lax.axis_index("cfg") == 0, guide[0], 1.0 - guide[0])
    for i, scalar in enumerate((factor, sig_now, sigma_of(step_index[0] + 1) - sig_now)):
        scalars[8 * i : 8 * i + 8, :] = jnp.full((8, 128), scalar, jnp.float32)
    copies[0].wait()
    fill_weight(weight, w_here, heads)
    for copy in copies[1:]:
        copy.wait()


def score_rows(heads, query, keys, refk, bias, exps_out):
    rows = query.shape[0]
    count, others = refk.shape[0], keys.shape[0]
    span = count + 128
    lane = lax.broadcasted_iota(jnp.int32, (rows, 128), 1)
    top_columns = jnp.zeros((rows, 128), jnp.float32)
    sum_columns = jnp.ones((rows, 128), jnp.float32)
    for first in range(0, heads, 8):
        some = range(first, first + 8)
        tops, exps, totals = head_exps(head_scores(query, keys, refk, bias[0:1], some))
        for h in some:
            start = h * span
            exps_out[:, start : start + count] = exps[h, 1].astype(jnp.bfloat16)
            start += count
            exps_out[:, start : start + others] = exps[h, 0].astype(jnp.bfloat16)
        top_columns = place_columns(top_columns, lane, tops)
        sum_columns = place_columns(sum_columns, lane, totals)
    top_columns = top_columns * SCALE
    return top_columns + jnp.log2(sum_columns), top_columns


def value_rows(heads, exps, values, refv, weight, out):
    count, others = refv.shape[0], values.shape[0]
    span = count + 128
    for first in range(0, heads, 16):
        some = range(first, first + 16)
        parts = {}
        for h in some:
            start = h * span
            parts[h, 1] = exps[:, start : start + count]
            parts[h, 0] = exps[:, start + count : start + count + others]
        outputs = head_outputs(parts, values, refv, some)
        for h in some:
            out[head_columns(h), :] = dot_t(weight[:, 2 * h * HD : 2 * (h + 1) * HD], outputs[h])


def early_scores_kernel(heads, own, near, k0, k1, refk, bias, exps, lse, top, keys, query):
    fill_rows(query, (own, near))
    fill_rows(keys, (k0, k1))
    lse[...], top[...] = score_rows(heads, query, keys, refk, bias, exps)


def early_values_kernel(heads, exps, v0, v1, refv, weight, out, values):
    fill_rows(values, (v0, v1))
    value_rows(heads, exps, values, refv, weight, out)


def late_scores_kernel(
    heads, mid_in, mid_out, far_in, far_out, keys, refk, bias, lse_early, top_early,
    exps, lse, top, query,
):
    @pl.when(is_inner())
    def _():
        fill_rows(query, (mid_in, far_in))

    @pl.when(jnp.logical_not(is_inner()))
    def _():
        fill_rows(query, (mid_out, far_out))

    low = lax.broadcasted_iota(jnp.int32, lse.shape, 1) < 64
    late = score_rows(heads, query, keys, refk, bias, exps)
    for out, early, mine in ((lse, lse_early, late[0]), (top, top_early, late[1])):
        out[...] = jnp.where(low, early[...], pltpu.roll(mine, 64, 1))


def late_values_kernel(heads, exps, values, refv, weight, out):
    value_rows(heads, exps, values, refv, weight, out)


def combine_kernel(
    heads, scalars, own, o1, o2, o3, top, early, late, b0, b1, b2, b3, velocity
):
    rows = own.shape[0]
    count = rows // 2
    everyone = [own[...]]
    for mask, ref in ((1, o1), (2, o2), (3, o3)):
        value = ref[...]
        if mask & 1:
            value = jnp.concatenate([value[count:], value[:count]], axis=0)
        if mask & 2:
            value = pltpu.roll(value, 64, 1)
        everyone.append(value)
    share = share_of(top[...], everyone) * scalars[0:1, :]
    turned = jnp.transpose(share)
    sums = []
    for base, parts in ((0, early), (64, late)):
        total = [None, None]
        for h in range(heads):
            for which in range(2):
                start = h * HD + which * 64
                row = base + which * 32 + h
                value = parts[start : start + 64, :] * turned[row : row + 1, :]
                total[h % 2] = value if total[h % 2] is None else total[h % 2] + value
        sums.append(total[0] + total[1])
    velocity[...] = jnp.transpose(jnp.concatenate(sums, axis=0))
    even = velocity[pl.ds(0, count, stride=2), :]
    odd = velocity[pl.ds(1, count, stride=2), :]
    low = lax.broadcasted_iota(jnp.int32, even.shape, 1) < 64
    first = jnp.where(low, even, pltpu.roll(odd, 64, 1))
    second = jnp.where(low, pltpu.roll(even, 64, 1), odd)
    half = count // 2
    b0[...], b1[...], b2[...], b3[...] = first[:half], first[half:], second[:half], second[half:]


def share_of(own, everyone):
    top = everyone[0]
    for value in everyone[1:]:
        top = jnp.maximum(top, value)
    total = jnp.exp2(everyone[0] - top)
    for value in everyone[1:]:
        total = total + jnp.exp2(value - top)
    return jnp.exp2(own - top) * (1.0 / total)


def split_kernel(b0, r1, r2, r3, kept, given):
    total = (b0[...] + r1[...]) + (r2[...] + r3[...])
    half = total.shape[0] // 2
    first = lax.axis_index("cfg") == 0
    kept[...] = jnp.where(first, total[:half], total[half:])
    given[...] = jnp.where(first, total[half:], total[:half])


def euler_kernel(scalars, latent, kept, taken, latent_next, denoised):
    guided = kept[...] + taken[...]
    latent_next[...] = latent[...] + scalars[16:17, :] * guided
    denoised[...] = latent[...] - scalars[8:9, :] * guided


def call(kernel, arrays, outs, scratch=(), mib=12, flops=0):
    return pl.pallas_call(
        kernel,
        in_specs=[VMEM] * len(arrays),
        out_specs=[VMEM] * len(outs),
        out_shape=outs,
        scratch_shapes=list(scratch),
        compiler_params=pltpu.CompilerParams(vmem_limit_bytes=mib << 20),
        cost_estimate=pl.CostEstimate(flops=flops, bytes_accessed=0, transcendentals=0),
    )(*[in_vmem(a) for a in arrays])


def line_of_four(
    query, keys, values, refk, refv, ref_len, step_index, guide, latent, w_t
):
    count, width = query.shape
    heads = width // HD
    rows, others = 2 * count, refk.shape[0]
    f32, bf16 = jnp.float32, jnp.bfloat16
    sources = (query, keys, values, refk, refv)
    k_other = swap(keys, "blk", 1)
    v_other = swap(values, "blk", 1)
    far_in = exchange(query, "seq", [(1, 2), (2, 1)])
    near = swap(query, "seq", 1)
    far_out = exchange(query, "seq", [(0, 3), (3, 0)])
    mid_in = exchange(query, "seq", [(0, 2), (3, 1)])
    mid_out = exchange(far_in, "seq", [(2, 3), (1, 0)])
    bias, scalars, query, keys, values, refk, refv, weight = pl.pallas_call(
        partial(load_kernel, heads),
        in_specs=[SMEM] * 3 + [pl.BlockSpec(memory_space=pltpu.HBM)] * 6,
        out_specs=[VMEM] * 8,
        out_shape=[pltpu.VMEM((8, others), f32), pltpu.VMEM((24, 128), f32)]
        + [pltpu.VMEM(a.shape, a.dtype) for a in sources]
        + [pltpu.VMEM((128, 2 * width), bf16)],
        scratch_shapes=[pltpu.VMEM(w_t.shape, w_t.dtype), pltpu.SemaphoreType.DMA((6,))],
        compiler_params=pltpu.CompilerParams(vmem_limit_bytes=2 << 20),
        cost_estimate=pl.CostEstimate(
            flops=10000000, bytes_accessed=4 * refk.size, transcendentals=0
        ),
        name="load",
    )(ref_len, step_index, guide, *[in_hbm(a) for a in (*sources, w_t)])
    exps_shape = pltpu.VMEM((rows, heads * (others + 128)), bf16)
    columns = pltpu.VMEM((rows, 128), f32)
    stacked = pltpu.VMEM((rows, width), bf16)
    partial_shape = pltpu.VMEM((width, rows), f32)
    flops = 2 * rows * (others + rows) * width
    exps_e, lse_e, top_e, keys = call(
        partial(early_scores_kernel, heads),
        (query, near, keys, k_other, refk, bias),
        [exps_shape, columns, columns, stacked], [stacked], flops=flops,
    )
    early, values = call(
        partial(early_values_kernel, heads),
        (exps_e, values, v_other, refv, weight), [partial_shape, stacked], flops=flops,
    )
    exps_l, lse, top = call(
        partial(late_scores_kernel, heads),
        (mid_in, mid_out, far_in, far_out, keys, refk, bias, lse_e, top_e),
        [exps_shape, columns, columns], [stacked], flops=flops,
    )
    o3 = swap(lse, "seq", 3)
    o2 = swap(lse, "seq", 2)
    o1 = swap(lse, "seq", 1)
    (late,) = call(
        partial(late_values_kernel, heads),
        (exps_l, values, refv, weight), [partial_shape], flops=flops,
    )
    block = pltpu.VMEM((count // 2, 128), f32)
    blocks = call(
        partial(combine_kernel, heads),
        (scalars, lse, o1, o2, o3, top, early, late), [block] * 4, [columns],
    )
    r3 = swap(blocks[3], "seq", 3)
    r2 = swap(blocks[2], "seq", 2)
    r1 = swap(blocks[1], "seq", 1)
    half = pltpu.VMEM(latent.shape, latent.dtype)
    kept, given = call(split_kernel, (blocks[0], r1, r2, r3), [half] * 2, mib=2)
    taken = swap(given, "cfg", 1)
    result = jax.ShapeDtypeStruct(latent.shape, latent.dtype)
    return call(euler_kernel, (scalars, latent, kept, taken), [result] * 2, mib=2)


def attend_kernel(heads, valid, query, keys, values, refk, refv, w_ref, out, lse, share, weight):
    step = pl.program_id(0)
    fill_weight(weight, w_ref, heads)
    index = lax.broadcasted_iota(jnp.int32, (1, refk.shape[0]), 1)
    bias = jnp.where(index < valid[0], 0.0, jnp.float32(NEG))
    lane = lax.broadcasted_iota(jnp.int32, lse.shape, 1)

    @pl.when(step == 0)
    def _():
        lse[...] = jnp.zeros_like(lse)
        share[...] = jnp.zeros_like(share)

    for h in range(heads):
        tops, exps, totals = head_exps(head_scores(query, keys, refk, bias, (h,)))
        exps = {item: value.astype(jnp.bfloat16) for item, value in exps.items()}
        outputs = head_outputs(exps, values, refv, (h,))
        out[:, head_columns(h)] = dot_t(outputs[h], weight[:, 2 * h * HD : 2 * (h + 1) * HD])
        for which in range(2):
            here = lane == which * 32 + step * heads + h
            top = tops[h, which] * SCALE
            share[...] = jnp.where(here, top, share[...])
            lse[...] = jnp.where(here, top + jnp.log2(totals[h, which]), lse[...])


def combine_any_kernel(heads, factor, top, everyone, parts, out, pairs):
    share = share_of(top[...], [everyone[i] for i in range(everyone.shape[0])])
    rows = share.shape[0]
    low = lax.broadcasted_iota(jnp.int32, (rows, 128), 1) < 64
    even = lax.broadcasted_iota(jnp.int32, (rows, 128), 0) % 2 == 0
    total = jnp.zeros((rows, 128), jnp.float32)
    for h in range(heads):
        both = jnp.where(low, share[:, h : h + 1], share[:, 32 + h : 33 + h])
        total += parts[:, head_columns(h)] * both
    total = total + pltpu.roll(total, 64, 1)
    pairs[...] = jnp.where(even == low, total * factor[0], 0.0)
    rows = out.shape[0]
    out[...] = pairs[pl.ds(0, rows, stride=2), :] + pairs[pl.ds(1, rows, stride=2), :]


def any_line(
    query, keys, values, refk, refv, ref_len, step_index, guide, latent, w_t
):
    line = lax.axis_size("seq")
    valid = ref_len - lax.axis_index("seq") * refk.shape[0]
    branch = lax.axis_index("cfg")
    factor = jnp.where(branch == 0, guide, 1.0 - guide)
    query = lax.all_gather(query, "seq", axis=0, tiled=True)
    keys = lax.all_gather(keys, "blk", axis=0, tiled=True)
    values = lax.all_gather(values, "blk", axis=0, tiled=True)
    rows, width = query.shape
    heads = width // HD
    some = 4
    columns = some * HD
    arrays = (query, keys, values, refk, refv, w_t)
    out, lse, top = pl.pallas_call(
        partial(attend_kernel, some),
        grid=(heads // some,),
        in_specs=[SMEM]
        + [pl.BlockSpec((a.shape[0], columns), lambda i: (0, i)) for a in arrays],
        out_specs=[
            pl.BlockSpec((rows, columns), lambda i: (0, i)),
            pl.BlockSpec((rows, 128), lambda i: (0, 0)),
            pl.BlockSpec((rows, 128), lambda i: (0, 0)),
        ],
        out_shape=[
            jax.ShapeDtypeStruct((rows, width), jnp.float32),
            jax.ShapeDtypeStruct((rows, 128), jnp.float32),
            jax.ShapeDtypeStruct((rows, 128), jnp.float32),
        ],
        scratch_shapes=[pltpu.VMEM((128, 2 * columns), jnp.bfloat16)],
        compiler_params=pltpu.CompilerParams(dimension_semantics=("arbitrary",)),
        name="attend",
    )(valid, *arrays)
    everyone = lax.all_gather(lse, "seq", axis=0, tiled=False)
    velocity = pl.pallas_call(
        partial(combine_any_kernel, heads),
        in_specs=[SMEM] + [VMEM] * 3,
        out_specs=VMEM,
        out_shape=jax.ShapeDtypeStruct((rows // 2, 128), jnp.float32),
        scratch_shapes=[pltpu.VMEM((rows, 128), jnp.float32)],
        name="combine",
    )(factor, top, everyone, out)
    blocks = velocity.reshape(line, -1, 128)
    mine = lax.all_to_all(blocks, "seq", split_axis=0, concat_axis=0, tiled=True).sum(0)
    half_rows = mine.shape[0] // 2
    kept = lax.dynamic_slice_in_dim(mine, branch * half_rows, half_rows, 0)
    given = lax.dynamic_slice_in_dim(mine, (1 - branch) * half_rows, half_rows, 0)
    guided = kept + swap(given, "cfg", 1)
    sig_now = sigma_of(step_index[0])
    sig_next = sigma_of(step_index[0] + 1)
    return (latent + (sig_next - sig_now) * guided, latent - sig_now * guided)


def on_device(
    queries, keys, values, ref_keys, ref_values, ref_len, step_index, guide, latent, w_out
):
    special = lax.axis_size("seq") == 4 and lax.axis_size("blk") == 2
    return tuple(
        (line_of_four if special else any_line)(
            queries[0], keys[0], values[0], ref_keys[0], ref_values[0],
            ref_len, step_index, guide, latent, w_out.T,
        )
    )


def solution(mesh):
    in_specs = (
        P(("groups", "cfg"), ("seq", "blk"), None),
        P(("groups", "cfg"), ("seq", "blk"), None),
        P(("groups", "cfg"), ("seq", "blk"), None),
        P(("groups", "cfg"), "seq", None),
        P(("groups", "cfg"), "seq", None),
        P(("groups", "cfg")),
        P("groups"),
        P("groups"),
        P(("groups", "seq", "blk", "cfg"), None),
        P(),
    )
    out_specs = (P(("groups", "seq", "blk", "cfg"), None), P(("groups", "seq", "blk", "cfg"), None))
    return jax.shard_map(
        on_device, mesh=mesh, in_specs=in_specs, out_specs=out_specs, check_vma=False
    )
```

```python
from functools import partial

import jax
import jax.numpy as jnp
from jax import lax
from jax.experimental import pallas as pl
from jax.experimental.pallas import tpu as pltpu
from jax.sharding import PartitionSpec as P

HD = 128
STEPS = 50
LOG2E = 1.4426950408889634
NEG = -1e30
SCALE = HD ** (-0.5) * LOG2E

SMEM = pl.BlockSpec(memory_space=pltpu.SMEM)
VMEM = pl.BlockSpec(memory_space=pltpu.VMEM)


def in_vmem(array):
    return pltpu.with_memory_space_constraint(array, pltpu.VMEM)


def in_hbm(array):
    return pltpu.with_memory_space_constraint(array, pltpu.HBM)


def dot_t(left, right):
    return lax.dot_general(
        left, right, (((1,), (1,)), ((), ())), preferred_element_type=jnp.float32
    )


def exchange(value, axis, pairs):
    return lax.ppermute(value, axis, pairs)


def swap(value, axis, mask):
    return exchange(value, axis, [(i, i ^ mask) for i in range(lax.axis_size(axis))])


def head_columns(head):
    return slice(head * HD, (head + 1) * HD)


def head_scores(query, keys, refkeys, bias, some):
    scores = {}
    for h in some:
        columns = head_columns(h)
        scores[h, 0] = dot_t(query[:, columns], keys[:, columns])
        scores[h, 1] = dot_t(query[:, columns], refkeys[:, columns]) + bias
    return scores


def head_exps(scores):
    tops = {item: jnp.max(score, axis=1, keepdims=True) for item, score in scores.items()}
    exps = {item: jnp.exp2((score - tops[item]) * SCALE) for item, score in scores.items()}
    totals = {item: jnp.sum(exps[item], axis=1, keepdims=True) for item in scores}
    return tops, exps, totals


def place_columns(target, lane, columns):
    for (h, which), column in columns.items():
        target = jnp.where(lane == which * 32 + h, column, target)
    return target


def head_outputs(exps, values, refvalues, some):
    return {
        h: jnp.concatenate(
            [
                jnp.dot(
                    exps[h, which], value[:, head_columns(h)], preferred_element_type=jnp.float32
                ).astype(jnp.bfloat16)
                for which, value in ((0, values), (1, refvalues))
            ],
            axis=1,
        )
        for h in some
    }


def fill_rows(scratch, refs):
    start = 0
    for ref in refs:
        scratch[start : start + ref.shape[0], :] = ref[...]
        start += ref.shape[0]


def fill_weight(weight, w_ref, heads):
    weight[...] = jnp.zeros_like(weight)
    out = w_ref.shape[0]
    for h in range(heads):
        weight[:out, 2 * h * HD : (2 * h + 1) * HD] = w_ref[:, head_columns(h)]
        weight[out:, (2 * h + 1) * HD : 2 * (h + 1) * HD] = w_ref[:, head_columns(h)]


def is_inner():
    place = lax.axis_index("seq")
    return jnp.logical_or(place == 1, place == 2)


def is_inner():
    place = lax.axis_index("seq")
    return jnp.logical_or(place == 1, place == 2)


def sigma_of(index):
    frac = 1.0 - index.astype(jnp.float32) / STEPS
    return 5.0 * frac / (1.0 + 4.0 * frac)


def load_kernel(heads, ref_len, step_index, guide, *refs):
    sources, w_ref, bias, scalars, targets, weight, w_here, sems = (
        refs[:5], refs[5], refs[6], refs[7], refs[8:13], refs[13], refs[14], refs[15]
    )
    copies = [
        pltpu.make_async_copy(source, target, sems.at[i])
        for i, (source, target) in enumerate(zip((w_ref, *sources), (w_here, *targets)))
    ]
    for copy in copies:
        copy.start()
    valid = ref_len[0] - lax.axis_index("seq") * sources[3].shape[0]
    index = lax.broadcasted_iota(jnp.int32, bias.shape, 1)
    bias[...] = jnp.where(index < valid, 0.0, jnp.float32(NEG))
    sig_now = sigma_of(step_index[0])
    factor = jnp.where(lax.axis_index("cfg") == 0, guide[0], 1.0 - guide[0])
    for i, scalar in enumerate((factor, sig_now, sigma_of(step_index[0] + 1) - sig_now)):
        scalars[8 * i : 8 * i + 8, :] = jnp.full((8, 128), scalar, jnp.float32)
    copies[0].wait()
    fill_weight(weight, w_here, heads)
    for copy in copies[1:]:
        copy.wait()


def score_rows(heads, query, keys, refk, bias, exps_out):
    rows = query.shape[0]
    count, others = refk.shape[0], keys.shape[0]
    span = count + 128
    lane = lax.broadcasted_iota(jnp.int32, (rows, 128), 1)
    top_columns = jnp.zeros((rows, 128), jnp.float32)
    sum_columns = jnp.ones((rows, 128), jnp.float32)
    for first in range(0, heads, 8):
        some = range(first, first + 8)
        tops, exps, totals = head_exps(head_scores(query, keys, refk, bias[0:1], some))
        for h in some:
            start = h * span
            exps_out[:, start : start + count] = exps[h, 1].astype(jnp.bfloat16)
            start += count
            exps_out[:, start : start + others] = exps[h, 0].astype(jnp.bfloat16)
        top_columns = place_columns(top_columns, lane, tops)
        sum_columns = place_columns(sum_columns, lane, totals)
    top_columns = top_columns * SCALE
    return top_columns + jnp.log2(sum_columns), top_columns


def value_rows(heads, exps, values, refv, weight, out):
    count, others = refv.shape[0], values.shape[0]
    span = count + 128
    for first in range(0, heads, 16):
        some = range(first, first + 16)
        parts = {}
        for h in some:
            start = h * span
            parts[h, 1] = exps[:, start : start + count]
            parts[h, 0] = exps[:, start + count : start + count + others]
        outputs = head_outputs(parts, values, refv, some)
        for h in some:
            out[head_columns(h), :] = dot_t(weight[:, 2 * h * HD : 2 * (h + 1) * HD], outputs[h])


def early_scores_kernel(heads, own, near, k0, k1, refk, bias, exps, lse, top, keys, query):
    fill_rows(query, (own, near))
    fill_rows(keys, (k0, k1))
    lse[...], top[...] = score_rows(heads, query, keys, refk, bias, exps)


def early_values_kernel(heads, exps, v0, v1, refv, weight, out, values):
    fill_rows(values, (v0, v1))
    value_rows(heads, exps, values, refv, weight, out)


def far_scores_kernel(heads, far_in, far_out, keys, refk, bias, exps, lse, top, query):
    @pl.when(is_inner())
    def _():
        query[...] = far_in[...]

    @pl.when(jnp.logical_not(is_inner()))
    def _():
        query[...] = far_out[...]

    lse[...], top[...] = score_rows(heads, query, keys, refk, bias, exps)


def middle_scores_kernel(
    heads, mid_in, mid_out, keys, refk, bias, lse_early, top_early, lse_far, top_far,
    exps, lse, top, query,
):
    @pl.when(is_inner())
    def _():
        query[...] = mid_in[...]

    @pl.when(jnp.logical_not(is_inner()))
    def _():
        query[...] = mid_out[...]

    count = query.shape[0]
    low = lax.broadcasted_iota(jnp.int32, (count, 128), 1) < 64
    far_lse, far_top = pltpu.roll(lse_far[...], 64, 1), pltpu.roll(top_far[...], 64, 1)
    lse[count:] = jnp.where(low, lse_early[count:], far_lse)
    top[count:] = jnp.where(low, top_early[count:], far_top)
    found = score_rows(heads, query, keys, refk, bias, exps)
    lse[:count] = jnp.where(low, lse_early[:count], pltpu.roll(found[0], 64, 1))
    top[:count] = jnp.where(low, top_early[:count], pltpu.roll(found[1], 64, 1))


def late_values_kernel(heads, middle, far, values, refv, weight, out, exps):
    fill_rows(exps, (middle, far))
    value_rows(heads, exps, values, refv, weight, out)


def combine_kernel(
    heads, scalars, own, o1, o2, o3, top, early, late, b0, b1, b2, b3, given, velocity
):
    rows = own.shape[0]
    count = rows // 2
    everyone = [own[...]]
    for mask, ref in ((1, o1), (2, o2), (3, o3)):
        value = ref[...]
        if mask & 1:
            value = jnp.concatenate([value[count:], value[:count]], axis=0)
        if mask & 2:
            value = pltpu.roll(value, 64, 1)
        everyone.append(value)
    share = share_of(top[...], everyone) * scalars[0:1, :]
    turned = jnp.transpose(share)
    sums = []
    for base, parts in ((0, early), (64, late)):
        total = [None, None]
        for h in range(heads):
            for which in range(2):
                start = h * HD + which * 64
                row = base + which * 32 + h
                value = parts[start : start + 64, :] * turned[row : row + 1, :]
                total[h % 2] = value if total[h % 2] is None else total[h % 2] + value
        sums.append(total[0] + total[1])
    velocity[...] = jnp.transpose(jnp.concatenate(sums, axis=0))
    even = velocity[pl.ds(0, count, stride=2), :]
    odd = velocity[pl.ds(1, count, stride=2), :]
    low = lax.broadcasted_iota(jnp.int32, even.shape, 1) < 64
    first = jnp.where(low, even, pltpu.roll(odd, 64, 1))
    second = jnp.where(low, pltpu.roll(even, 64, 1), odd)
    half = count // 2
    blocks = first[:half], first[half:], second[:half], second[half:]
    cfg = lax.axis_index("cfg") == 0
    size = half // 2
    for i, (block, kept) in enumerate(zip(blocks, (b0, b1, b2, b3))):
        kept[...] = jnp.where(cfg, block[:size], block[size:])
        given[i * 16 : i * 16 + size, :] = jnp.where(cfg, block[size:], block[:size])


def share_of(own, everyone):
    top = everyone[0]
    for value in everyone[1:]:
        top = jnp.maximum(top, value)
    total = jnp.exp2(everyone[0] - top)
    for value in everyone[1:]:
        total = total + jnp.exp2(value - top)
    return jnp.exp2(own - top) * (1.0 / total)


def join_kernel(taken, b0, b1, b2, b3, g0, g1, g2, g3):
    for i, (block, out) in enumerate(((b0, g0), (b1, g1), (b2, g2), (b3, g3))):
        out[...] = block[...] + taken[i * 16 : i * 16 + out.shape[0], :]


def euler_kernel(scalars, latent, own, r1, r2, r3, latent_next, denoised):
    guided = (own[...] + r1[...]) + (r2[...] + r3[...])
    latent_next[...] = latent[...] + scalars[16:17, :] * guided
    denoised[...] = latent[...] - scalars[8:9, :] * guided


def call(kernel, arrays, outs, scratch=(), mib=12, flops=0):
    return pl.pallas_call(
        kernel,
        in_specs=[VMEM] * len(arrays),
        out_specs=[VMEM] * len(outs),
        out_shape=outs,
        scratch_shapes=list(scratch),
        compiler_params=pltpu.CompilerParams(vmem_limit_bytes=mib << 20),
        cost_estimate=pl.CostEstimate(flops=flops, bytes_accessed=0, transcendentals=0),
    )(*[in_vmem(a) for a in arrays])


def line_of_four(
    query, keys, values, refk, refv, ref_len, step_index, guide, latent, w_t
):
    count, width = query.shape
    heads = width // HD
    rows, others = 2 * count, refk.shape[0]
    f32, bf16 = jnp.float32, jnp.bfloat16
    sources = (query, keys, values, refk, refv)
    k_other = swap(keys, "blk", 1)
    v_other = swap(values, "blk", 1)
    far_in = exchange(query, "seq", [(1, 2), (2, 1)])
    near = swap(query, "seq", 1)
    far_out = exchange(query, "seq", [(0, 3), (3, 0)])
    mid_in = exchange(query, "seq", [(0, 2), (3, 1)])
    mid_out = exchange(far_in, "seq", [(2, 3), (1, 0)])
    bias, scalars, query, keys, values, refk, refv, weight = pl.pallas_call(
        partial(load_kernel, heads),
        in_specs=[SMEM] * 3 + [pl.BlockSpec(memory_space=pltpu.HBM)] * 6,
        out_specs=[VMEM] * 8,
        out_shape=[pltpu.VMEM((8, others), f32), pltpu.VMEM((24, 128), f32)]
        + [pltpu.VMEM(a.shape, a.dtype) for a in sources]
        + [pltpu.VMEM((128, 2 * width), bf16)],
        scratch_shapes=[pltpu.VMEM(w_t.shape, w_t.dtype), pltpu.SemaphoreType.DMA((6,))],
        compiler_params=pltpu.CompilerParams(vmem_limit_bytes=2 << 20),
        cost_estimate=pl.CostEstimate(
            flops=10000000, bytes_accessed=4 * refk.size, transcendentals=0
        ),
        name="load",
    )(ref_len, step_index, guide, *[in_hbm(a) for a in (*sources, w_t)])
    exps_shape = pltpu.VMEM((rows, heads * (others + 128)), bf16)
    columns = pltpu.VMEM((rows, 128), f32)
    stacked = pltpu.VMEM((rows, width), bf16)
    partial_shape = pltpu.VMEM((width, rows), f32)
    flops = 2 * rows * (others + rows) * width
    exps_e, lse_e, top_e, keys = call(
        partial(early_scores_kernel, heads),
        (query, near, keys, k_other, refk, bias),
        [exps_shape, columns, columns, stacked], [stacked], flops=flops,
    )
    early, values = call(
        partial(early_values_kernel, heads),
        (exps_e, values, v_other, refv, weight), [partial_shape, stacked], flops=flops,
    )
    small = pltpu.VMEM((count, exps_shape.shape[1]), bf16)
    column = pltpu.VMEM((count, 128), f32)
    block_shape = pltpu.VMEM((count, width), bf16)
    exps_f, lse_f, top_f = call(
        partial(far_scores_kernel, heads),
        (far_in, far_out, keys, refk, bias),
        [small, column, column], [block_shape], flops=flops // 2,
    )
    exps_m, lse, top = call(
        partial(middle_scores_kernel, heads),
        (mid_in, mid_out, keys, refk, bias, lse_e, top_e, lse_f, top_f),
        [small, columns, columns], [block_shape], flops=flops // 2,
    )
    o3 = swap(lse, "seq", 3)
    o2 = swap(lse, "seq", 2)
    o1 = swap(lse, "seq", 1)
    (late,) = call(
        partial(late_values_kernel, heads),
        (exps_m, exps_f, values, refv, weight), [partial_shape], [exps_shape], flops=flops,
    )
    half = pltpu.VMEM(latent.shape, f32)
    *kept, given = call(
        partial(combine_kernel, heads),
        (scalars, lse, o1, o2, o3, top, early, late),
        [half] * 4 + [pltpu.VMEM((64, 128), f32)], [columns],
    )
    taken = swap(given, "cfg", 1)
    blocks = call(join_kernel, (taken, *kept), [half] * 4, mib=2)
    r3 = swap(blocks[3], "seq", 3)
    r2 = swap(blocks[2], "seq", 2)
    r1 = swap(blocks[1], "seq", 1)
    result = jax.ShapeDtypeStruct(latent.shape, latent.dtype)
    return call(euler_kernel, (scalars, latent, blocks[0], r1, r2, r3), [result] * 2, mib=2)


def attend_kernel(heads, valid, query, keys, values, refk, refv, w_ref, out, lse, share, weight):
    step = pl.program_id(0)
    fill_weight(weight, w_ref, heads)
    index = lax.broadcasted_iota(jnp.int32, (1, refk.shape[0]), 1)
    bias = jnp.where(index < valid[0], 0.0, jnp.float32(NEG))
    lane = lax.broadcasted_iota(jnp.int32, lse.shape, 1)

    @pl.when(step == 0)
    def _():
        lse[...] = jnp.zeros_like(lse)
        share[...] = jnp.zeros_like(share)

    for h in range(heads):
        tops, exps, totals = head_exps(head_scores(query, keys, refk, bias, (h,)))
        exps = {item: value.astype(jnp.bfloat16) for item, value in exps.items()}
        outputs = head_outputs(exps, values, refv, (h,))
        out[:, head_columns(h)] = dot_t(outputs[h], weight[:, 2 * h * HD : 2 * (h + 1) * HD])
        for which in range(2):
            here = lane == which * 32 + step * heads + h
            top = tops[h, which] * SCALE
            share[...] = jnp.where(here, top, share[...])
            lse[...] = jnp.where(here, top + jnp.log2(totals[h, which]), lse[...])


def combine_any_kernel(heads, factor, top, everyone, parts, out, pairs):
    share = share_of(top[...], [everyone[i] for i in range(everyone.shape[0])])
    rows = share.shape[0]
    low = lax.broadcasted_iota(jnp.int32, (rows, 128), 1) < 64
    even = lax.broadcasted_iota(jnp.int32, (rows, 128), 0) % 2 == 0
    total = jnp.zeros((rows, 128), jnp.float32)
    for h in range(heads):
        both = jnp.where(low, share[:, h : h + 1], share[:, 32 + h : 33 + h])
        total += parts[:, head_columns(h)] * both
    total = total + pltpu.roll(total, 64, 1)
    pairs[...] = jnp.where(even == low, total * factor[0], 0.0)
    rows = out.shape[0]
    out[...] = pairs[pl.ds(0, rows, stride=2), :] + pairs[pl.ds(1, rows, stride=2), :]


def any_line(
    query, keys, values, refk, refv, ref_len, step_index, guide, latent, w_t
):
    line = lax.axis_size("seq")
    valid = ref_len - lax.axis_index("seq") * refk.shape[0]
    branch = lax.axis_index("cfg")
    factor = jnp.where(branch == 0, guide, 1.0 - guide)
    query = lax.all_gather(query, "seq", axis=0, tiled=True)
    keys = lax.all_gather(keys, "blk", axis=0, tiled=True)
    values = lax.all_gather(values, "blk", axis=0, tiled=True)
    rows, width = query.shape
    heads = width // HD
    some = 4
    columns = some * HD
    arrays = (query, keys, values, refk, refv, w_t)
    out, lse, top = pl.pallas_call(
        partial(attend_kernel, some),
        grid=(heads // some,),
        in_specs=[SMEM]
        + [pl.BlockSpec((a.shape[0], columns), lambda i: (0, i)) for a in arrays],
        out_specs=[
            pl.BlockSpec((rows, columns), lambda i: (0, i)),
            pl.BlockSpec((rows, 128), lambda i: (0, 0)),
            pl.BlockSpec((rows, 128), lambda i: (0, 0)),
        ],
        out_shape=[
            jax.ShapeDtypeStruct((rows, width), jnp.float32),
            jax.ShapeDtypeStruct((rows, 128), jnp.float32),
            jax.ShapeDtypeStruct((rows, 128), jnp.float32),
        ],
        scratch_shapes=[pltpu.VMEM((128, 2 * columns), jnp.bfloat16)],
        compiler_params=pltpu.CompilerParams(dimension_semantics=("arbitrary",)),
        name="attend",
    )(valid, *arrays)
    everyone = lax.all_gather(lse, "seq", axis=0, tiled=False)
    velocity = pl.pallas_call(
        partial(combine_any_kernel, heads),
        in_specs=[SMEM] + [VMEM] * 3,
        out_specs=VMEM,
        out_shape=jax.ShapeDtypeStruct((rows // 2, 128), jnp.float32),
        scratch_shapes=[pltpu.VMEM((rows, 128), jnp.float32)],
        name="combine",
    )(factor, top, everyone, out)
    blocks = velocity.reshape(line, -1, 128)
    mine = lax.all_to_all(blocks, "seq", split_axis=0, concat_axis=0, tiled=True).sum(0)
    half_rows = mine.shape[0] // 2
    kept = lax.dynamic_slice_in_dim(mine, branch * half_rows, half_rows, 0)
    given = lax.dynamic_slice_in_dim(mine, (1 - branch) * half_rows, half_rows, 0)
    guided = kept + swap(given, "cfg", 1)
    sig_now = sigma_of(step_index[0])
    sig_next = sigma_of(step_index[0] + 1)
    return (latent + (sig_next - sig_now) * guided, latent - sig_now * guided)


def on_device(
    queries, keys, values, ref_keys, ref_values, ref_len, step_index, guide, latent, w_out
):
    special = lax.axis_size("seq") == 4 and lax.axis_size("blk") == 2
    return tuple(
        (line_of_four if special else any_line)(
            queries[0], keys[0], values[0], ref_keys[0], ref_values[0],
            ref_len, step_index, guide, latent, w_out.T,
        )
    )


def solution(mesh):
    in_specs = (
        P(("groups", "cfg"), ("seq", "blk"), None),
        P(("groups", "cfg"), ("seq", "blk"), None),
        P(("groups", "cfg"), ("seq", "blk"), None),
        P(("groups", "cfg"), "seq", None),
        P(("groups", "cfg"), "seq", None),
        P(("groups", "cfg")),
        P("groups"),
        P("groups"),
        P(("groups", "seq", "blk", "cfg"), None),
        P(),
    )
    out_specs = (P(("groups", "seq", "blk", "cfg"), None), P(("groups", "seq", "blk", "cfg"), None))
    return jax.shard_map(
        on_device, mesh=mesh, in_specs=in_specs, out_specs=out_specs, check_vma=False
    )
```

```python
from functools import partial

import jax
import jax.numpy as jnp
from jax import lax
from jax.experimental import pallas as pl
from jax.experimental.pallas import tpu as pltpu
from jax.sharding import PartitionSpec as P

HD = 128
STEPS = 50
LOG2E = 1.4426950408889634
NEG = -1e30
SCALE = HD ** (-0.5) * LOG2E

SMEM = pl.BlockSpec(memory_space=pltpu.SMEM)
VMEM = pl.BlockSpec(memory_space=pltpu.VMEM)


def in_vmem(array):
    return pltpu.with_memory_space_constraint(array, pltpu.VMEM)


def in_hbm(array):
    return pltpu.with_memory_space_constraint(array, pltpu.HBM)


def dot_t(left, right):
    return lax.dot_general(
        left, right, (((1,), (1,)), ((), ())), preferred_element_type=jnp.float32
    )


def exchange(value, axis, pairs):
    return lax.ppermute(value, axis, pairs)


def swap(value, axis, mask):
    return exchange(value, axis, [(i, i ^ mask) for i in range(lax.axis_size(axis))])


def head_columns(head):
    return slice(head * HD, (head + 1) * HD)


def head_scores(query, keys, refkeys, bias, some, turned=False):
    scores = {}
    for h in some:
        columns = head_columns(h)
        scores[h, 0] = dot_t(query[:, columns], keys[:, columns])
        if turned:
            found = jnp.dot(
                query[:, columns], refkeys[columns, :], preferred_element_type=jnp.float32
            )
        else:
            found = dot_t(query[:, columns], refkeys[:, columns])
        scores[h, 1] = found + bias
    return scores


def head_exps(scores):
    tops = {item: jnp.max(score, axis=1, keepdims=True) for item, score in scores.items()}
    exps = {item: jnp.exp2((score - tops[item]) * SCALE) for item, score in scores.items()}
    totals = {item: jnp.sum(exps[item], axis=1, keepdims=True) for item in scores}
    return tops, exps, totals


def place_columns(target, lane, columns):
    for (h, which), column in columns.items():
        target = jnp.where(lane == which * 32 + h, column, target)
    return target


def head_outputs(exps, values, refvalues, some):
    return {
        h: jnp.concatenate(
            [
                jnp.dot(
                    exps[h, which], value[:, head_columns(h)], preferred_element_type=jnp.float32
                ).astype(jnp.bfloat16)
                for which, value in ((0, values), (1, refvalues))
            ],
            axis=1,
        )
        for h in some
    }


def fill_rows(scratch, refs):
    start = 0
    for ref in refs:
        scratch[start : start + ref.shape[0], :] = ref[...]
        start += ref.shape[0]


def fill_weight(weight, w_ref, heads):
    weight[...] = jnp.zeros_like(weight)
    out = w_ref.shape[0]
    for h in range(heads):
        weight[:out, 2 * h * HD : (2 * h + 1) * HD] = w_ref[:, head_columns(h)]
        weight[out:, (2 * h + 1) * HD : 2 * (h + 1) * HD] = w_ref[:, head_columns(h)]


def is_inner():
    place = lax.axis_index("seq")
    return jnp.logical_or(place == 1, place == 2)


def is_inner():
    place = lax.axis_index("seq")
    return jnp.logical_or(place == 1, place == 2)


def sigma_of(index):
    frac = 1.0 - index.astype(jnp.float32) / STEPS
    return 5.0 * frac / (1.0 + 4.0 * frac)


def load_kernel(heads, ref_len, step_index, guide, *refs):
    refk, sources, w_ref, bias, scalars, turned, targets, weight, w_here, refk_here, sems = (
        refs[0], refs[1:5], refs[5], refs[6], refs[7], refs[8], refs[9:13], *refs[13:]
    )
    copies = [
        pltpu.make_async_copy(source, target, sems.at[i])
        for i, (source, target) in enumerate(
            zip((w_ref, refk, *sources), (w_here, refk_here, *targets))
        )
    ]
    for copy in copies:
        copy.start()
    valid = ref_len[0] - lax.axis_index("seq") * refk.shape[0]
    index = lax.broadcasted_iota(jnp.int32, bias.shape, 1)
    bias[...] = jnp.where(index < valid, 0.0, jnp.float32(NEG))
    sig_now = sigma_of(step_index[0])
    factor = jnp.where(lax.axis_index("cfg") == 0, guide[0], 1.0 - guide[0])
    for i, scalar in enumerate((factor, sig_now, sigma_of(step_index[0] + 1) - sig_now)):
        scalars[8 * i : 8 * i + 8, :] = jnp.full((8, 128), scalar, jnp.float32)
    copies[0].wait()
    fill_weight(weight, w_here, heads)
    copies[1].wait()
    for h in range(heads):
        turned[head_columns(h), :] = jnp.transpose(refk_here[:, head_columns(h)])
    for copy in copies[2:]:
        copy.wait()


def score_rows(heads, query, keys, refk, bias, exps_out):
    rows = query.shape[0]
    count, others = refk.shape[1], keys.shape[0]
    span = count + 128
    lane = lax.broadcasted_iota(jnp.int32, (rows, 128), 1)
    top_columns = jnp.zeros((rows, 128), jnp.float32)
    sum_columns = jnp.ones((rows, 128), jnp.float32)
    for first in range(0, heads, 8):
        some = range(first, first + 8)
        tops, exps, totals = head_exps(head_scores(query, keys, refk, bias[0:1], some, True))
        for h in some:
            start = h * span
            exps_out[:, start : start + count] = exps[h, 1].astype(jnp.bfloat16)
            start += count
            exps_out[:, start : start + others] = exps[h, 0].astype(jnp.bfloat16)
        top_columns = place_columns(top_columns, lane, tops)
        sum_columns = place_columns(sum_columns, lane, totals)
    top_columns = top_columns * SCALE
    return top_columns + jnp.log2(sum_columns), top_columns


def value_rows(heads, exps, values, refv, weight, out):
    count, others = refv.shape[0], values.shape[0]
    span = count + 128
    for first in range(0, heads, 16):
        some = range(first, first + 16)
        parts = {}
        for h in some:
            start = h * span
            parts[h, 1] = exps[:, start : start + count]
            parts[h, 0] = exps[:, start + count : start + count + others]
        outputs = head_outputs(parts, values, refv, some)
        for h in some:
            out[head_columns(h), :] = dot_t(weight[:, 2 * h * HD : 2 * (h + 1) * HD], outputs[h])


def early_scores_kernel(heads, own, near, k0, k1, refk, bias, exps, lse, top, keys, query):
    fill_rows(query, (own, near))
    fill_rows(keys, (k0, k1))
    lse[...], top[...] = score_rows(heads, query, keys, refk, bias, exps)


def early_values_kernel(heads, exps, v0, v1, refv, weight, out, values):
    fill_rows(values, (v0, v1))
    value_rows(heads, exps, values, refv, weight, out)


def far_scores_kernel(heads, far_in, far_out, keys, refk, bias, exps, lse, top, query):
    @pl.when(is_inner())
    def _():
        query[...] = far_in[...]

    @pl.when(jnp.logical_not(is_inner()))
    def _():
        query[...] = far_out[...]

    lse[...], top[...] = score_rows(heads, query, keys, refk, bias, exps)


def middle_scores_kernel(
    heads, mid_in, mid_out, keys, refk, bias, lse_early, top_early, lse_far, top_far,
    exps, lse, top, query,
):
    @pl.when(is_inner())
    def _():
        query[...] = mid_in[...]

    @pl.when(jnp.logical_not(is_inner()))
    def _():
        query[...] = mid_out[...]

    count = query.shape[0]
    low = lax.broadcasted_iota(jnp.int32, (count, 128), 1) < 64
    far_lse, far_top = pltpu.roll(lse_far[...], 64, 1), pltpu.roll(top_far[...], 64, 1)
    lse[count:] = jnp.where(low, lse_early[count:], far_lse)
    top[count:] = jnp.where(low, top_early[count:], far_top)
    found = score_rows(heads, query, keys, refk, bias, exps)
    lse[:count] = jnp.where(low, lse_early[:count], pltpu.roll(found[0], 64, 1))
    top[:count] = jnp.where(low, top_early[:count], pltpu.roll(found[1], 64, 1))


def late_values_kernel(heads, middle, far, values, refv, weight, out, exps):
    fill_rows(exps, (middle, far))
    value_rows(heads, exps, values, refv, weight, out)


def combine_kernel(
    heads, scalars, own, o1, o2, o3, top, early, late, mine, across, side, given, velocity
):
    rows = own.shape[0]
    count = rows // 2
    everyone = [own[...]]
    for mask, ref in ((1, o1), (2, o2), (3, o3)):
        value = ref[...]
        if mask & 1:
            value = jnp.concatenate([value[count:], value[:count]], axis=0)
        if mask & 2:
            value = pltpu.roll(value, 64, 1)
        everyone.append(value)
    share = share_of(top[...], everyone) * scalars[0:1, :]
    turned = jnp.transpose(share)
    sums = []
    for base, parts in ((0, early), (64, late)):
        total = [None, None]
        for h in range(heads):
            for which in range(2):
                start = h * HD + which * 64
                row = base + which * 32 + h
                value = parts[start : start + 64, :] * turned[row : row + 1, :]
                total[h % 2] = value if total[h % 2] is None else total[h % 2] + value
        sums.append(total[0] + total[1])
    velocity[...] = jnp.transpose(jnp.concatenate(sums, axis=0))
    even = velocity[pl.ds(0, count, stride=2), :]
    odd = velocity[pl.ds(1, count, stride=2), :]
    low = lax.broadcasted_iota(jnp.int32, even.shape, 1) < 64
    first = jnp.where(low, even, pltpu.roll(odd, 64, 1))
    second = jnp.where(low, pltpu.roll(even, 64, 1), odd)
    half = count // 2
    size = half // 2
    blocks = first[:half], first[half:], second[:half], second[half:]
    cfg = lax.axis_index("cfg") == 0
    side[...] = jnp.where(cfg, blocks[1], blocks[3])
    given[:half] = jnp.where(cfg, blocks[3], blocks[1])
    for i, kept in ((0, mine), (2, across)):
        kept[...] = jnp.where(cfg, blocks[i][:size], blocks[i][size:])
        start = 24 + 8 * i
        given[start : start + size] = jnp.where(cfg, blocks[i][size:], blocks[i][:size])


def share_of(own, everyone):
    top = everyone[0]
    for value in everyone[1:]:
        top = jnp.maximum(top, value)
    total = jnp.exp2(everyone[0] - top)
    for value in everyone[1:]:
        total = total + jnp.exp2(value - top)
    return jnp.exp2(own - top) * (1.0 / total)


def join_kernel(taken, mine, across, side, mine_out, across_out, side_out):
    rows, size = side.shape[0], mine.shape[0]
    side_out[...] = side[...] + taken[:rows]
    mine_out[...] = mine[...] + taken[24 : 24 + size]
    across_out[...] = across[...] + taken[40 : 40 + size]


def euler_kernel(scalars, latent, mine, across, side, other, latent_next, denoised):
    size = mine.shape[0]
    sides = side[...] + other[...]
    sides = jnp.where(lax.axis_index("cfg") == 0, sides[:size], sides[size:])
    guided = (mine[...] + across[...]) + sides
    latent_next[...] = latent[...] + scalars[16:17, :] * guided
    denoised[...] = latent[...] - scalars[8:9, :] * guided


def call(kernel, arrays, outs, scratch=(), mib=12, flops=0):
    return pl.pallas_call(
        kernel,
        in_specs=[VMEM] * len(arrays),
        out_specs=[VMEM] * len(outs),
        out_shape=outs,
        scratch_shapes=list(scratch),
        compiler_params=pltpu.CompilerParams(vmem_limit_bytes=mib << 20),
        cost_estimate=pl.CostEstimate(flops=flops, bytes_accessed=0, transcendentals=0),
    )(*[in_vmem(a) for a in arrays])


def line_of_four(
    query, keys, values, refk, refv, ref_len, step_index, guide, latent, w_t
):
    count, width = query.shape
    heads = width // HD
    rows, others = 2 * count, refk.shape[0]
    f32, bf16 = jnp.float32, jnp.bfloat16
    sources = (query, keys, values, refv)
    k_other = swap(keys, "blk", 1)
    v_other = swap(values, "blk", 1)
    far_in = exchange(query, "seq", [(1, 2), (2, 1)])
    near = swap(query, "seq", 1)
    far_out = exchange(query, "seq", [(0, 3), (3, 0)])
    mid_in = exchange(query, "seq", [(0, 2), (3, 1)])
    mid_out = exchange(far_in, "seq", [(2, 3), (1, 0)])
    bias, scalars, refk, query, keys, values, refv, weight = pl.pallas_call(
        partial(load_kernel, heads),
        in_specs=[SMEM] * 3 + [pl.BlockSpec(memory_space=pltpu.HBM)] * 6,
        out_specs=[VMEM] * 8,
        out_shape=[pltpu.VMEM((8, others), f32), pltpu.VMEM((24, 128), f32)]
        + [pltpu.VMEM((width, others), bf16)]
        + [pltpu.VMEM(a.shape, a.dtype) for a in sources]
        + [pltpu.VMEM((128, 2 * width), bf16)],
        scratch_shapes=[
            pltpu.VMEM(w_t.shape, w_t.dtype),
            pltpu.VMEM(refk.shape, refk.dtype),
            pltpu.SemaphoreType.DMA((6,)),
        ],
        compiler_params=pltpu.CompilerParams(vmem_limit_bytes=6 << 20),
        cost_estimate=pl.CostEstimate(
            flops=10000000, bytes_accessed=4 * refk.size, transcendentals=0
        ),
        name="load",
    )(ref_len, step_index, guide, *[in_hbm(a) for a in (refk, *sources, w_t)])
    exps_shape = pltpu.VMEM((rows, heads * (others + 128)), bf16)
    columns = pltpu.VMEM((rows, 128), f32)
    stacked = pltpu.VMEM((rows, width), bf16)
    partial_shape = pltpu.VMEM((width, rows), f32)
    flops = 2 * rows * (others + rows) * width
    exps_e, lse_e, top_e, keys = call(
        partial(early_scores_kernel, heads),
        (query, near, keys, k_other, refk, bias),
        [exps_shape, columns, columns, stacked], [stacked], flops=flops,
    )
    early, values = call(
        partial(early_values_kernel, heads),
        (exps_e, values, v_other, refv, weight), [partial_shape, stacked], flops=flops,
    )
    small = pltpu.VMEM((count, exps_shape.shape[1]), bf16)
    column = pltpu.VMEM((count, 128), f32)
    block_shape = pltpu.VMEM((count, width), bf16)
    exps_f, lse_f, top_f = call(
        partial(far_scores_kernel, heads),
        (far_in, far_out, keys, refk, bias),
        [small, column, column], [block_shape], flops=flops // 2,
    )
    exps_m, lse, top = call(
        partial(middle_scores_kernel, heads),
        (mid_in, mid_out, keys, refk, bias, lse_e, top_e, lse_f, top_f),
        [small, columns, columns], [block_shape], flops=flops // 2,
    )
    o3 = swap(lse, "seq", 3)
    o2 = swap(lse, "seq", 2)
    o1 = swap(lse, "seq", 1)
    (late,) = call(
        partial(late_values_kernel, heads),
        (exps_m, exps_f, values, refv, weight), [partial_shape], [exps_shape], flops=flops,
    )
    half = pltpu.VMEM(latent.shape, f32)
    whole = pltpu.VMEM((count // 2, 128), f32)
    *kept, given = call(
        partial(combine_kernel, heads),
        (scalars, lse, o1, o2, o3, top, early, late),
        [half, half, whole, pltpu.VMEM((56, 128), f32)], [columns],
    )
    taken = swap(given, "cfg", 1)
    mine, across, side = call(join_kernel, (taken, *kept), [half, half, whole], mib=2)
    pairs = [(2 * z, 2 * (z ^ 1)) for z in range(4)]
    pairs += [(2 * z + 1, 2 * (z ^ 3) + 1) for z in range(4)]
    side = exchange(side, ("seq", "cfg"), pairs)
    across = swap(across, "seq", 2)
    other = swap(side, "cfg", 1)
    result = jax.ShapeDtypeStruct(latent.shape, latent.dtype)
    return call(euler_kernel, (scalars, latent, mine, across, side, other), [result] * 2, mib=2)


def attend_kernel(heads, valid, query, keys, values, refk, refv, w_ref, out, lse, share, weight):
    step = pl.program_id(0)
    fill_weight(weight, w_ref, heads)
    index = lax.broadcasted_iota(jnp.int32, (1, refk.shape[0]), 1)
    bias = jnp.where(index < valid[0], 0.0, jnp.float32(NEG))
    lane = lax.broadcasted_iota(jnp.int32, lse.shape, 1)

    @pl.when(step == 0)
    def _():
        lse[...] = jnp.zeros_like(lse)
        share[...] = jnp.zeros_like(share)

    for h in range(heads):
        tops, exps, totals = head_exps(head_scores(query, keys, refk, bias, (h,)))
        exps = {item: value.astype(jnp.bfloat16) for item, value in exps.items()}
        outputs = head_outputs(exps, values, refv, (h,))
        out[:, head_columns(h)] = dot_t(outputs[h], weight[:, 2 * h * HD : 2 * (h + 1) * HD])
        for which in range(2):
            here = lane == which * 32 + step * heads + h
            top = tops[h, which] * SCALE
            share[...] = jnp.where(here, top, share[...])
            lse[...] = jnp.where(here, top + jnp.log2(totals[h, which]), lse[...])


def combine_any_kernel(heads, factor, top, everyone, parts, out, pairs):
    share = share_of(top[...], [everyone[i] for i in range(everyone.shape[0])])
    rows = share.shape[0]
    low = lax.broadcasted_iota(jnp.int32, (rows, 128), 1) < 64
    even = lax.broadcasted_iota(jnp.int32, (rows, 128), 0) % 2 == 0
    total = jnp.zeros((rows, 128), jnp.float32)
    for h in range(heads):
        both = jnp.where(low, share[:, h : h + 1], share[:, 32 + h : 33 + h])
        total += parts[:, head_columns(h)] * both
    total = total + pltpu.roll(total, 64, 1)
    pairs[...] = jnp.where(even == low, total * factor[0], 0.0)
    rows = out.shape[0]
    out[...] = pairs[pl.ds(0, rows, stride=2), :] + pairs[pl.ds(1, rows, stride=2), :]


def any_line(
    query, keys, values, refk, refv, ref_len, step_index, guide, latent, w_t
):
    line = lax.axis_size("seq")
    valid = ref_len - lax.axis_index("seq") * refk.shape[0]
    branch = lax.axis_index("cfg")
    factor = jnp.where(branch == 0, guide, 1.0 - guide)
    query = lax.all_gather(query, "seq", axis=0, tiled=True)
    keys = lax.all_gather(keys, "blk", axis=0, tiled=True)
    values = lax.all_gather(values, "blk", axis=0, tiled=True)
    rows, width = query.shape
    heads = width // HD
    some = 4
    columns = some * HD
    arrays = (query, keys, values, refk, refv, w_t)
    out, lse, top = pl.pallas_call(
        partial(attend_kernel, some),
        grid=(heads // some,),
        in_specs=[SMEM]
        + [pl.BlockSpec((a.shape[0], columns), lambda i: (0, i)) for a in arrays],
        out_specs=[
            pl.BlockSpec((rows, columns), lambda i: (0, i)),
            pl.BlockSpec((rows, 128), lambda i: (0, 0)),
            pl.BlockSpec((rows, 128), lambda i: (0, 0)),
        ],
        out_shape=[
            jax.ShapeDtypeStruct((rows, width), jnp.float32),
            jax.ShapeDtypeStruct((rows, 128), jnp.float32),
            jax.ShapeDtypeStruct((rows, 128), jnp.float32),
        ],
        scratch_shapes=[pltpu.VMEM((128, 2 * columns), jnp.bfloat16)],
        compiler_params=pltpu.CompilerParams(dimension_semantics=("arbitrary",)),
        name="attend",
    )(valid, *arrays)
    everyone = lax.all_gather(lse, "seq", axis=0, tiled=False)
    velocity = pl.pallas_call(
        partial(combine_any_kernel, heads),
        in_specs=[SMEM] + [VMEM] * 3,
        out_specs=VMEM,
        out_shape=jax.ShapeDtypeStruct((rows // 2, 128), jnp.float32),
        scratch_shapes=[pltpu.VMEM((rows, 128), jnp.float32)],
        name="combine",
    )(factor, top, everyone, out)
    blocks = velocity.reshape(line, -1, 128)
    mine = lax.all_to_all(blocks, "seq", split_axis=0, concat_axis=0, tiled=True).sum(0)
    half_rows = mine.shape[0] // 2
    kept = lax.dynamic_slice_in_dim(mine, branch * half_rows, half_rows, 0)
    given = lax.dynamic_slice_in_dim(mine, (1 - branch) * half_rows, half_rows, 0)
    guided = kept + swap(given, "cfg", 1)
    sig_now = sigma_of(step_index[0])
    sig_next = sigma_of(step_index[0] + 1)
    return (latent + (sig_next - sig_now) * guided, latent - sig_now * guided)


def on_device(
    queries, keys, values, ref_keys, ref_values, ref_len, step_index, guide, latent, w_out
):
    special = lax.axis_size("seq") == 4 and lax.axis_size("blk") == 2
    return tuple(
        (line_of_four if special else any_line)(
            queries[0], keys[0], values[0], ref_keys[0], ref_values[0],
            ref_len, step_index, guide, latent, w_out.T,
        )
    )


def solution(mesh):
    in_specs = (
        P(("groups", "cfg"), ("seq", "blk"), None),
        P(("groups", "cfg"), ("seq", "blk"), None),
        P(("groups", "cfg"), ("seq", "blk"), None),
        P(("groups", "cfg"), "seq", None),
        P(("groups", "cfg"), "seq", None),
        P(("groups", "cfg")),
        P("groups"),
        P("groups"),
        P(("groups", "seq", "blk", "cfg"), None),
        P(),
    )
    out_specs = (P(("groups", "seq", "blk", "cfg"), None), P(("groups", "seq", "blk", "cfg"), None))
    return jax.shard_map(
        on_device, mesh=mesh, in_specs=in_specs, out_specs=out_specs, check_vma=False
    )
```

```python
from functools import partial

import jax
import jax.numpy as jnp
from jax import lax
from jax.experimental import pallas as pl
from jax.experimental.pallas import tpu as pltpu
from jax.sharding import PartitionSpec as P

HD = 128
STEPS = 50
LOG2E = 1.4426950408889634
NEG = -1e30
SCALE = HD ** (-0.5) * LOG2E

SMEM = pl.BlockSpec(memory_space=pltpu.SMEM)
VMEM = pl.BlockSpec(memory_space=pltpu.VMEM)


def in_vmem(array):
    return pltpu.with_memory_space_constraint(array, pltpu.VMEM)


def in_hbm(array):
    return pltpu.with_memory_space_constraint(array, pltpu.HBM)


def dot_t(left, right):
    return lax.dot_general(
        left, right, (((1,), (1,)), ((), ())), preferred_element_type=jnp.float32
    )


def exchange(value, axis, pairs):
    return lax.ppermute(value, axis, pairs)


def swap(value, axis, mask):
    return exchange(value, axis, [(i, i ^ mask) for i in range(lax.axis_size(axis))])


def head_columns(head):
    return slice(head * HD, (head + 1) * HD)


def head_scores(query, keys, refkeys, bias, some, base=0, turned=False):
    scores = {}
    for h in some:
        columns = head_columns(h)
        here = query[:, head_columns(h - base)]
        scores[h, 0] = dot_t(here, keys[:, columns])
        if turned:
            found = jnp.dot(here, refkeys[columns, :], preferred_element_type=jnp.float32)
        else:
            found = dot_t(here, refkeys[:, columns])
        scores[h, 1] = found + bias
    return scores


def head_exps(scores):
    tops = {item: jnp.max(score, axis=1, keepdims=True) for item, score in scores.items()}
    exps = {item: jnp.exp2((score - tops[item]) * SCALE) for item, score in scores.items()}
    totals = {item: jnp.sum(exps[item], axis=1, keepdims=True) for item in scores}
    return tops, exps, totals


def place_columns(target, lane, columns):
    for (h, which), column in columns.items():
        target = jnp.where(lane == which * 32 + h, column, target)
    return target


def head_outputs(exps, values, refvalues, some):
    return {
        h: jnp.concatenate(
            [
                jnp.dot(
                    exps[h, which], value[:, head_columns(h)], preferred_element_type=jnp.float32
                ).astype(jnp.bfloat16)
                for which, value in ((0, values), (1, refvalues))
            ],
            axis=1,
        )
        for h in some
    }


def fill_rows(scratch, refs):
    start = 0
    for ref in refs:
        scratch[start : start + ref.shape[0], :] = ref[...]
        start += ref.shape[0]


def fill_weight(weight, w_ref, heads):
    weight[...] = jnp.zeros_like(weight)
    out = w_ref.shape[0]
    for h in range(heads):
        weight[:out, 2 * h * HD : (2 * h + 1) * HD] = w_ref[:, head_columns(h)]
        weight[out:, (2 * h + 1) * HD : 2 * (h + 1) * HD] = w_ref[:, head_columns(h)]


def is_inner():
    place = lax.axis_index("seq")
    return jnp.logical_or(place == 1, place == 2)


def is_inner():
    place = lax.axis_index("seq")
    return jnp.logical_or(place == 1, place == 2)


def sigma_of(index):
    frac = 1.0 - index.astype(jnp.float32) / STEPS
    return 5.0 * frac / (1.0 + 4.0 * frac)


def load_kernel(heads, ref_len, step_index, guide, *refs):
    refk, sources, w_ref, bias, scalars, turned, targets, weight, w_here, refk_here, sems = (
        refs[0], refs[1:5], refs[5], refs[6], refs[7], refs[8], refs[9:13], *refs[13:]
    )
    copies = [
        pltpu.make_async_copy(source, target, sems.at[i])
        for i, (source, target) in enumerate(
            zip((w_ref, refk, *sources), (w_here, refk_here, *targets))
        )
    ]
    for copy in copies:
        copy.start()
    valid = ref_len[0] - lax.axis_index("seq") * refk.shape[0]
    index = lax.broadcasted_iota(jnp.int32, bias.shape, 1)
    bias[...] = jnp.where(index < valid, 0.0, jnp.float32(NEG))
    sig_now = sigma_of(step_index[0])
    factor = jnp.where(lax.axis_index("cfg") == 0, guide[0], 1.0 - guide[0])
    for i, scalar in enumerate((factor, sig_now, sigma_of(step_index[0] + 1) - sig_now)):
        scalars[8 * i : 8 * i + 8, :] = jnp.full((8, 128), scalar, jnp.float32)
    copies[0].wait()
    fill_weight(weight, w_here, heads)
    copies[1].wait()
    for h in range(heads):
        turned[head_columns(h), :] = jnp.transpose(refk_here[:, head_columns(h)])
    for copy in copies[2:]:
        copy.wait()


def score_rows(heads, query, keys, refk, bias, exps_out, base=0):
    rows = query.shape[0]
    count, others = refk.shape[1], keys.shape[0]
    span = count + 128
    lane = lax.broadcasted_iota(jnp.int32, (rows, 128), 1)
    top_columns = jnp.zeros((rows, 128), jnp.float32)
    sum_columns = jnp.ones((rows, 128), jnp.float32)
    for first in range(base, base + heads, 8):
        some = range(first, first + 8)
        scores = head_scores(query, keys, refk, bias[0:1], some, base, True)
        tops, exps, totals = head_exps(scores)
        for h in some:
            start = (h - base) * span
            exps_out[:, start : start + count] = exps[h, 1].astype(jnp.bfloat16)
            start += count
            exps_out[:, start : start + others] = exps[h, 0].astype(jnp.bfloat16)
        top_columns = place_columns(top_columns, lane, tops)
        sum_columns = place_columns(sum_columns, lane, totals)
    top_columns = top_columns * SCALE
    return top_columns + jnp.log2(sum_columns), top_columns


def value_rows(heads, exps, values, refv, weight, out):
    count, others = refv.shape[0], values.shape[0]
    span = count + 128
    for first in range(0, heads, 16):
        some = range(first, first + 16)
        parts = {}
        for h in some:
            start = h * span
            parts[h, 1] = exps[:, start : start + count]
            parts[h, 0] = exps[:, start + count : start + count + others]
        outputs = head_outputs(parts, values, refv, some)
        for h in some:
            out[head_columns(h), :] = dot_t(weight[:, 2 * h * HD : 2 * (h + 1) * HD], outputs[h])


def early_scores_kernel(heads, own, near, k0, k1, refk, bias, exps, lse, top, keys, query):
    fill_rows(query, (own, near))
    fill_rows(keys, (k0, k1))
    lse[...], top[...] = score_rows(heads, query, keys, refk, bias, exps)


def early_values_kernel(heads, exps, v0, v1, refv, weight, out, values):
    fill_rows(values, (v0, v1))
    value_rows(heads, exps, values, refv, weight, out)


def far_scores_kernel(heads, far_in, far_out, keys, refk, bias, exps, lse, top, query):
    @pl.when(is_inner())
    def _():
        query[...] = far_in[...]

    @pl.when(jnp.logical_not(is_inner()))
    def _():
        query[...] = far_out[...]

    lse[...], top[...] = score_rows(heads, query, keys, refk, bias, exps)


def cut_kernel(source, left, right):
    half = left.shape[1]
    left[...] = source[:, :half]
    right[...] = source[:, half:]


def cut_hbm_kernel(source, left, right, sems):
    half = left.shape[1]
    copies = [
        pltpu.make_async_copy(source.at[:, pl.ds(i * half, out.shape[1])], out, sems.at[i])
        for i, out in enumerate((left, right))
    ]
    for copy in copies:
        copy.start()
    for copy in copies:
        copy.wait()


def fill_middle(query, mid_in, mid_out):
    @pl.when(is_inner())
    def _():
        query[...] = mid_in[...]

    @pl.when(jnp.logical_not(is_inner()))
    def _():
        query[...] = mid_out[...]


def middle_first_kernel(heads, mid_in, mid_out, keys, refk, bias, exps, lse, top, query):
    fill_middle(query, mid_in, mid_out)
    lse[...], top[...] = score_rows(heads, query, keys, refk, bias, exps)


def middle_second_kernel(
    base, heads, mid_in, mid_out, keys, refk, bias, lse_early, top_early, lse_far, top_far,
    lse_first, top_first, exps, lse, top, query,
):
    fill_middle(query, mid_in, mid_out)
    count = query.shape[0]
    lane = lax.broadcasted_iota(jnp.int32, (count, 128), 1)
    low = lane < 64
    far_lse, far_top = pltpu.roll(lse_far[...], 64, 1), pltpu.roll(top_far[...], 64, 1)
    lse[count:] = jnp.where(low, lse_early[count:], far_lse)
    top[count:] = jnp.where(low, top_early[count:], far_top)
    found = score_rows(heads, query, keys, refk, bias, exps, base)
    before = lane % 32 < base
    for out, early, first, second in (
        (lse, lse_early, lse_first, found[0]), (top, top_early, top_first, found[1]),
    ):
        both = jnp.where(before, first[...], second)
        out[:count] = jnp.where(low, early[:count], pltpu.roll(both, 64, 1))


def late_values_kernel(heads, first, second, far, values, refv, weight, out, exps):
    count, half = first.shape
    exps[:count, :half] = first[...]
    exps[:count, half:] = second[...]
    exps[count:] = far[...]
    value_rows(heads, exps, values, refv, weight, out)


def combine_kernel(
    heads, scalars, own, o1, o2, o3, top, early, late, mine, across, side, given, velocity
):
    rows = own.shape[0]
    count = rows // 2
    everyone = [own[...]]
    for mask, ref in ((1, o1), (2, o2), (3, o3)):
        value = ref[...]
        if mask & 1:
            value = jnp.concatenate([value[count:], value[:count]], axis=0)
        if mask & 2:
            value = pltpu.roll(value, 64, 1)
        everyone.append(value)
    share = share_of(top[...], everyone) * scalars[0:1, :]
    turned = jnp.transpose(share)
    sums = []
    for base, parts in ((0, early), (64, late)):
        total = [None, None]
        for h in range(heads):
            for which in range(2):
                start = h * HD + which * 64
                row = base + which * 32 + h
                value = parts[start : start + 64, :] * turned[row : row + 1, :]
                total[h % 2] = value if total[h % 2] is None else total[h % 2] + value
        sums.append(total[0] + total[1])
    velocity[...] = jnp.transpose(jnp.concatenate(sums, axis=0))
    even = velocity[pl.ds(0, count, stride=2), :]
    odd = velocity[pl.ds(1, count, stride=2), :]
    low = lax.broadcasted_iota(jnp.int32, even.shape, 1) < 64
    first = jnp.where(low, even, pltpu.roll(odd, 64, 1))
    second = jnp.where(low, pltpu.roll(even, 64, 1), odd)
    half = count // 2
    size = half // 2
    blocks = first[:half], first[half:], second[:half], second[half:]
    cfg = lax.axis_index("cfg") == 0
    side[...] = jnp.where(cfg, blocks[1], blocks[3])
    given[:half] = jnp.where(cfg, blocks[3], blocks[1])
    for i, kept in ((0, mine), (2, across)):
        kept[...] = jnp.where(cfg, blocks[i][:size], blocks[i][size:])
        start = 24 + 8 * i
        given[start : start + size] = jnp.where(cfg, blocks[i][size:], blocks[i][:size])


def share_of(own, everyone):
    top = everyone[0]
    for value in everyone[1:]:
        top = jnp.maximum(top, value)
    total = jnp.exp2(everyone[0] - top)
    for value in everyone[1:]:
        total = total + jnp.exp2(value - top)
    return jnp.exp2(own - top) * (1.0 / total)


def join_kernel(taken, mine, across, side, mine_out, across_out, side_out):
    rows, size = side.shape[0], mine.shape[0]
    side_out[...] = side[...] + taken[:rows]
    mine_out[...] = mine[...] + taken[24 : 24 + size]
    across_out[...] = across[...] + taken[40 : 40 + size]


def euler_kernel(scalars, latent, mine, across, side, other, latent_next, denoised):
    size = mine.shape[0]
    sides = side[...] + other[...]
    sides = jnp.where(lax.axis_index("cfg") == 0, sides[:size], sides[size:])
    guided = (mine[...] + across[...]) + sides
    latent_next[...] = latent[...] + scalars[16:17, :] * guided
    denoised[...] = latent[...] - scalars[8:9, :] * guided


def call(kernel, arrays, outs, scratch=(), mib=12, flops=0):
    return pl.pallas_call(
        kernel,
        in_specs=[VMEM] * len(arrays),
        out_specs=[VMEM] * len(outs),
        out_shape=outs,
        scratch_shapes=list(scratch),
        compiler_params=pltpu.CompilerParams(vmem_limit_bytes=mib << 20),
        cost_estimate=pl.CostEstimate(flops=flops, bytes_accessed=0, transcendentals=0),
    )(*[in_vmem(a) for a in arrays])


def line_of_four(
    query, keys, values, refk, refv, ref_len, step_index, guide, latent, w_t
):
    count, width = query.shape
    heads = width // HD
    rows, others = 2 * count, refk.shape[0]
    f32, bf16 = jnp.float32, jnp.bfloat16
    sources = (query, keys, values, refv)
    k_other = swap(keys, "blk", 1)
    v_other = swap(values, "blk", 1)
    far_in = exchange(query, "seq", [(1, 2), (2, 1)])
    near = swap(query, "seq", 1)
    far_out = exchange(query, "seq", [(0, 3), (3, 0)])
    ahead = heads - heads // 4
    part_shapes = [
        pltpu.VMEM((count, ahead * HD), bf16),
        pltpu.VMEM((count, width - ahead * HD), bf16),
    ]
    own_parts = pl.pallas_call(
        cut_hbm_kernel,
        in_specs=[pl.BlockSpec(memory_space=pltpu.HBM)],
        out_specs=[VMEM] * 2,
        out_shape=part_shapes,
        scratch_shapes=[pltpu.SemaphoreType.DMA((2,))],
        compiler_params=pltpu.CompilerParams(vmem_limit_bytes=2 << 20),
        name="cut_own",
    )(in_hbm(query))
    mid_in_first = exchange(own_parts[0], "seq", [(0, 2), (3, 1)])
    mid_in_second = exchange(own_parts[1], "seq", [(0, 2), (3, 1)])
    far_parts = call(cut_kernel, (far_in,), part_shapes, mib=2)
    mid_out_first = exchange(far_parts[0], "seq", [(2, 3), (1, 0)])
    mid_out_second = exchange(far_parts[1], "seq", [(2, 3), (1, 0)])
    bias, scalars, refk, query, keys, values, refv, weight = pl.pallas_call(
        partial(load_kernel, heads),
        in_specs=[SMEM] * 3 + [pl.BlockSpec(memory_space=pltpu.HBM)] * 6,
        out_specs=[VMEM] * 8,
        out_shape=[pltpu.VMEM((8, others), f32), pltpu.VMEM((24, 128), f32)]
        + [pltpu.VMEM((width, others), bf16)]
        + [pltpu.VMEM(a.shape, a.dtype) for a in sources]
        + [pltpu.VMEM((128, 2 * width), bf16)],
        scratch_shapes=[
            pltpu.VMEM(w_t.shape, w_t.dtype),
            pltpu.VMEM(refk.shape, refk.dtype),
            pltpu.SemaphoreType.DMA((6,)),
        ],
        compiler_params=pltpu.CompilerParams(vmem_limit_bytes=6 << 20),
        cost_estimate=pl.CostEstimate(
            flops=10000000, bytes_accessed=4 * refk.size, transcendentals=0
        ),
        name="load",
    )(ref_len, step_index, guide, *[in_hbm(a) for a in (refk, *sources, w_t)])
    exps_shape = pltpu.VMEM((rows, heads * (others + 128)), bf16)
    columns = pltpu.VMEM((rows, 128), f32)
    stacked = pltpu.VMEM((rows, width), bf16)
    partial_shape = pltpu.VMEM((width, rows), f32)
    flops = 2 * rows * (others + rows) * width
    exps_e, lse_e, top_e, keys = call(
        partial(early_scores_kernel, heads),
        (query, near, keys, k_other, refk, bias),
        [exps_shape, columns, columns, stacked], [stacked], flops=flops,
    )
    early, values = call(
        partial(early_values_kernel, heads),
        (exps_e, values, v_other, refv, weight), [partial_shape, stacked], flops=flops,
    )
    small = pltpu.VMEM((count, exps_shape.shape[1]), bf16)
    column = pltpu.VMEM((count, 128), f32)
    block_shape = pltpu.VMEM((count, width), bf16)
    exps_f, lse_f, top_f = call(
        partial(far_scores_kernel, heads),
        (far_in, far_out, keys, refk, bias),
        [small, column, column], [block_shape], flops=flops // 2,
    )
    cuts = [pltpu.VMEM((count, n * (others + 128)), bf16) for n in (ahead, heads - ahead)]
    exps_m, lse_m, top_m = call(
        partial(middle_first_kernel, ahead),
        (mid_in_first, mid_out_first, keys, refk, bias),
        [cuts[0], column, column], part_shapes[:1], flops=flops // 4,
    )
    exps_n, lse, top = call(
        partial(middle_second_kernel, ahead, heads - ahead),
        (
            mid_in_second, mid_out_second, keys, refk, bias,
            lse_e, top_e, lse_f, top_f, lse_m, top_m,
        ),
        [cuts[1], columns, columns], part_shapes[1:], flops=flops // 4,
    )
    o3 = swap(lse, "seq", 3)
    o2 = swap(lse, "seq", 2)
    o1 = swap(lse, "seq", 1)
    (late,) = call(
        partial(late_values_kernel, heads),
        (exps_m, exps_n, exps_f, values, refv, weight),
        [partial_shape], [exps_shape], flops=flops,
    )
    half = pltpu.VMEM(latent.shape, f32)
    whole = pltpu.VMEM((count // 2, 128), f32)
    *kept, given = call(
        partial(combine_kernel, heads),
        (scalars, lse, o1, o2, o3, top, early, late),
        [half, half, whole, pltpu.VMEM((56, 128), f32)], [columns],
    )
    taken = swap(given, "cfg", 1)
    mine, across, side = call(join_kernel, (taken, *kept), [half, half, whole], mib=2)
    pairs = [(2 * z, 2 * (z ^ 1)) for z in range(4)]
    pairs += [(2 * z + 1, 2 * (z ^ 3) + 1) for z in range(4)]
    side = exchange(side, ("seq", "cfg"), pairs)
    across = swap(across, "seq", 2)
    other = swap(side, "cfg", 1)
    result = jax.ShapeDtypeStruct(latent.shape, latent.dtype)
    return call(euler_kernel, (scalars, latent, mine, across, side, other), [result] * 2, mib=2)


def attend_kernel(heads, valid, query, keys, values, refk, refv, w_ref, out, lse, share, weight):
    step = pl.program_id(0)
    fill_weight(weight, w_ref, heads)
    index = lax.broadcasted_iota(jnp.int32, (1, refk.shape[0]), 1)
    bias = jnp.where(index < valid[0], 0.0, jnp.float32(NEG))
    lane = lax.broadcasted_iota(jnp.int32, lse.shape, 1)

    @pl.when(step == 0)
    def _():
        lse[...] = jnp.zeros_like(lse)
        share[...] = jnp.zeros_like(share)

    for h in range(heads):
        tops, exps, totals = head_exps(head_scores(query, keys, refk, bias, (h,)))
        exps = {item: value.astype(jnp.bfloat16) for item, value in exps.items()}
        outputs = head_outputs(exps, values, refv, (h,))
        out[:, head_columns(h)] = dot_t(outputs[h], weight[:, 2 * h * HD : 2 * (h + 1) * HD])
        for which in range(2):
            here = lane == which * 32 + step * heads + h
            top = tops[h, which] * SCALE
            share[...] = jnp.where(here, top, share[...])
            lse[...] = jnp.where(here, top + jnp.log2(totals[h, which]), lse[...])


def combine_any_kernel(heads, factor, top, everyone, parts, out, pairs):
    share = share_of(top[...], [everyone[i] for i in range(everyone.shape[0])])
    rows = share.shape[0]
    low = lax.broadcasted_iota(jnp.int32, (rows, 128), 1) < 64
    even = lax.broadcasted_iota(jnp.int32, (rows, 128), 0) % 2 == 0
    total = jnp.zeros((rows, 128), jnp.float32)
    for h in range(heads):
        both = jnp.where(low, share[:, h : h + 1], share[:, 32 + h : 33 + h])
        total += parts[:, head_columns(h)] * both
    total = total + pltpu.roll(total, 64, 1)
    pairs[...] = jnp.where(even == low, total * factor[0], 0.0)
    rows = out.shape[0]
    out[...] = pairs[pl.ds(0, rows, stride=2), :] + pairs[pl.ds(1, rows, stride=2), :]


def any_line(
    query, keys, values, refk, refv, ref_len, step_index, guide, latent, w_t
):
    line = lax.axis_size("seq")
    valid = ref_len - lax.axis_index("seq") * refk.shape[0]
    branch = lax.axis_index("cfg")
    factor = jnp.where(branch == 0, guide, 1.0 - guide)
    query = lax.all_gather(query, "seq", axis=0, tiled=True)
    keys = lax.all_gather(keys, "blk", axis=0, tiled=True)
    values = lax.all_gather(values, "blk", axis=0, tiled=True)
    rows, width = query.shape
    heads = width // HD
    some = 4
    columns = some * HD
    arrays = (query, keys, values, refk, refv, w_t)
    out, lse, top = pl.pallas_call(
        partial(attend_kernel, some),
        grid=(heads // some,),
        in_specs=[SMEM]
        + [pl.BlockSpec((a.shape[0], columns), lambda i: (0, i)) for a in arrays],
        out_specs=[
            pl.BlockSpec((rows, columns), lambda i: (0, i)),
            pl.BlockSpec((rows, 128), lambda i: (0, 0)),
            pl.BlockSpec((rows, 128), lambda i: (0, 0)),
        ],
        out_shape=[
            jax.ShapeDtypeStruct((rows, width), jnp.float32),
            jax.ShapeDtypeStruct((rows, 128), jnp.float32),
            jax.ShapeDtypeStruct((rows, 128), jnp.float32),
        ],
        scratch_shapes=[pltpu.VMEM((128, 2 * columns), jnp.bfloat16)],
        compiler_params=pltpu.CompilerParams(dimension_semantics=("arbitrary",)),
        name="attend",
    )(valid, *arrays)
    everyone = lax.all_gather(lse, "seq", axis=0, tiled=False)
    velocity = pl.pallas_call(
        partial(combine_any_kernel, heads),
        in_specs=[SMEM] + [VMEM] * 3,
        out_specs=VMEM,
        out_shape=jax.ShapeDtypeStruct((rows // 2, 128), jnp.float32),
        scratch_shapes=[pltpu.VMEM((rows, 128), jnp.float32)],
        name="combine",
    )(factor, top, everyone, out)
    blocks = velocity.reshape(line, -1, 128)
    mine = lax.all_to_all(blocks, "seq", split_axis=0, concat_axis=0, tiled=True).sum(0)
    half_rows = mine.shape[0] // 2
    kept = lax.dynamic_slice_in_dim(mine, branch * half_rows, half_rows, 0)
    given = lax.dynamic_slice_in_dim(mine, (1 - branch) * half_rows, half_rows, 0)
    guided = kept + swap(given, "cfg", 1)
    sig_now = sigma_of(step_index[0])
    sig_next = sigma_of(step_index[0] + 1)
    return (latent + (sig_next - sig_now) * guided, latent - sig_now * guided)


def on_device(
    queries, keys, values, ref_keys, ref_values, ref_len, step_index, guide, latent, w_out
):
    special = lax.axis_size("seq") == 4 and lax.axis_size("blk") == 2
    return tuple(
        (line_of_four if special else any_line)(
            queries[0], keys[0], values[0], ref_keys[0], ref_values[0],
            ref_len, step_index, guide, latent, w_out.T,
        )
    )


def solution(mesh):
    in_specs = (
        P(("groups", "cfg"), ("seq", "blk"), None),
        P(("groups", "cfg"), ("seq", "blk"), None),
        P(("groups", "cfg"), ("seq", "blk"), None),
        P(("groups", "cfg"), "seq", None),
        P(("groups", "cfg"), "seq", None),
        P(("groups", "cfg")),
        P("groups"),
        P("groups"),
        P(("groups", "seq", "blk", "cfg"), None),
        P(),
    )
    out_specs = (P(("groups", "seq", "blk", "cfg"), None), P(("groups", "seq", "blk", "cfg"), None))
    return jax.shard_map(
        on_device, mesh=mesh, in_specs=in_specs, out_specs=out_specs, check_vma=False
    )
```
